32 devices in a mesh: dp: 2 (over z, core), tp: 16 (over x, y).
Axes of the slice: x: 4, y: 4, z: 1, core: 2. Of those that a mesh axis runs over, the one named last changes fastest.
The devices are a block of a 4x4x8 slice.
Arguments:
- x: bfloat16 [5120, 7168], P(('dp', 'tp')), parts along dimension 0
- dy: bfloat16 [5120, 7168], P(('dp', 'tp')), parts along dimension 0
- pre: bfloat16 [5120, 28672], P('dp', 'tp'), parts along dimension 0
- w_in: bfloat16 [7168, 28672], P(None, 'tp')
- w_down: bfloat16 [28672, 7168], P('tp')
Outputs:
- output 1: bfloat16 [5120, 7168], P(('dp', 'tp')), parts along dimension 0
- output 2: bfloat16 [14336, 28672], P('dp', 'tp'), parts along dimension 0
- output 3: bfloat16 [57344, 7168], P(('dp', 'tp')), parts along dimension 0
There are 2 independent parts. The reference program is written for one: setup_inputs(seed, part) draws one part's arguments, and reference() takes and returns one part's arrays. A program takes and returns all parts, laid end to end along the dimension named above; an argument that names none is the same for every part.
All inputs are finite; a program needn't handle non-finite values.
Results may differ from the reference program's by a relative error of at most 0.012.
Values are sent between devices in bfloat16 or wider.
A program may use at most 768 MiB of HBM per device.

```python
import jax
import jax.numpy as jnp

ROWS = 2560
D = 7168
FF = 28672


def act(pre):
    return jax.nn.gelu(pre)


def setup_inputs(seed: int = 0, part: int = 0) -> dict:
    kx, ky, ka, ki, kd = jax.random.split(jax.random.key(seed), 5)
    kx, ky, ka = (jax.random.fold_in(k, part) for k in (kx, ky, ka))
    drawn = {
        "x": jax.random.normal(kx, (ROWS, D), jnp.float32),
        "dy": jax.random.normal(ky, (ROWS, D), jnp.float32),
        "pre": jax.random.normal(ka, (ROWS, FF), jnp.float32),
        "w_in": jax.random.normal(ki, (D, FF), jnp.float32) * D**-0.5,
        "w_down": jax.random.normal(kd, (FF, D), jnp.float32) * FF**-0.5,
    }
    return {k: v.astype(jnp.bfloat16) for k, v in drawn.items()}


def reference(x, dy, pre, w_in, w_down):
    hidden, back = jax.vjp(act, pre.astype(jnp.float32))
    d_hidden = jnp.dot(dy, w_down.T, preferred_element_type=jnp.float32)
    d_pre = back(d_hidden)[0].astype(jnp.bfloat16)
    dx = jnp.dot(d_pre, w_in.T, preferred_element_type=jnp.float32)
    dw_in = jnp.dot(x.T, d_pre, preferred_element_type=jnp.float32)
    dw_down = jnp.dot(hidden.astype(jnp.bfloat16).T, dy, preferred_element_type=jnp.float32)
    return tuple(g.astype(jnp.bfloat16) for g in (dx, dw_in, dw_down))
```

```python
import jax
import jax.numpy as jnp
from jax import lax
from jax.experimental import pallas as pl
from jax.experimental.pallas import tpu as pltpu
from jax.sharding import PartitionSpec as P


def act(pre):
    return jax.nn.gelu(pre)


def tn_kernel(a_ref, b_ref, o_ref):
    o_ref[...] = lax.dot_general(
        a_ref[...], b_ref[...], (((0,), (0,)), ((), ())), preferred_element_type=jnp.float32
    ).astype(o_ref.dtype)


def tn_matmul(a, b, tile):
    rows, columns = a.shape
    width = b.shape[1]
    return pl.pallas_call(
        tn_kernel,
        grid=(columns // tile,),
        in_specs=[
            pl.BlockSpec((rows, tile), lambda i: (0, i)),
            pl.BlockSpec((rows, width), lambda i: (0, 0)),
        ],
        out_specs=pl.BlockSpec((tile, width), lambda i: (i, 0)),
        out_shape=jax.ShapeDtypeStruct((columns, width), a.dtype),
        compiler_params=pltpu.CompilerParams(vmem_limit_bytes=60 * 1024 * 1024),
        cost_estimate=pl.CostEstimate(
            flops=2 * rows * columns * width,
            bytes_accessed=2 * (rows * columns + rows * width + columns * width),
            transcendentals=0,
        ),
        name="tn_matmul",
    )(a, b)


def solution(mesh):
    def step(x, dy, pre, w_in, w_down):
        dy_all = lax.all_gather(dy, "tp", tiled=True)
        x, dy_all = lax.optimization_barrier((x, dy_all))
        x_all = lax.all_gather(x, "tp", tiled=True)
        hidden, back = jax.vjp(act, pre.astype(jnp.float32))
        d_hidden = jnp.dot(dy_all, w_down.T, preferred_element_type=jnp.float32)
        d_pre = back(d_hidden)[0].astype(jnp.bfloat16)
        dx = jnp.dot(d_pre, w_in.T, preferred_element_type=jnp.float32).astype(jnp.bfloat16)
        dx = lax.psum_scatter(dx, "tp", tiled=True)
        dw_down = jnp.dot(hidden.astype(jnp.bfloat16).T, dy_all, preferred_element_type=jnp.float32)
        return dx, tn_matmul(x_all, d_pre, 512), dw_down.astype(jnp.bfloat16)

    tokens = P(("dp", "tp"), None)
    return jax.shard_map(
        step,
        mesh=mesh,
        in_specs=(tokens, tokens, P("dp", "tp"), P(None, "tp"), P("tp", None)),
        out_specs=(tokens, P("dp", "tp"), tokens),
        check_vma=False,
    )
```

```python
import functools
import math

import jax
import jax.numpy as jnp
from jax import lax
from jax.experimental import pallas as pl
from jax.experimental.pallas import tpu as pltpu
from jax.sharding import PartitionSpec as P

MESH = pl.DeviceIdType.MESH
TILE = 256


def act(pre):
    return jax.nn.gelu(pre)


def tn_kernel(a_ref, b_ref, o_ref):
    o_ref[...] = lax.dot_general(
        a_ref[...], b_ref[...], (((0,), (0,)), ((), ())), preferred_element_type=jnp.float32
    ).astype(o_ref.dtype)


def tn_matmul(a, b, tile, tile_b=False):
    rows, height = a.shape
    width = b.shape[1]
    whole, cut = lambda i: (0, 0), lambda i: (0, i)
    return pl.pallas_call(
        tn_kernel,
        grid=((width if tile_b else height) // tile,),
        in_specs=[
            pl.BlockSpec((rows, height if tile_b else tile), whole if tile_b else cut),
            pl.BlockSpec((rows, tile if tile_b else width), cut if tile_b else whole),
        ],
        out_specs=pl.BlockSpec((height, tile) if tile_b else (tile, width), cut if tile_b else lambda i: (i, 0)),
        out_shape=jax.ShapeDtypeStruct((height, width), a.dtype),
        compiler_params=pltpu.CompilerParams(vmem_limit_bytes=60 * 1024 * 1024),
        cost_estimate=pl.CostEstimate(
            flops=2 * rows * height * width,
            bytes_accessed=2 * (rows * height + rows * width + height * width),
            transcendentals=0,
        ),
        name="tn_matmul",
    )(a, b)


STEPS = ((1, 0), (-1, 0), (0, 1), (0, -1))


def pieces_of(link):
    along_x, up = link < 2, link % 2 == 0
    mine = (0, 1) if along_x else (2, 3)
    other = (2, 3) if along_x else (0, 1)
    if not up:
        mine, other = mine[::-1], other[::-1]
    back = -1 if up else 1

    def at(first, second):
        return (first, second) if along_x else (second, first)

    return (
        [(*at(0, 0), q) for q in mine + other],
        [(*at(back, 0), mine[0])],
        [(*at(0, s), q) for s, order in ((-1, (0, 1)), (1, (1, 0))) for q in (min(other) + order[0], min(other) + order[1])],
        [(*at(0, 2), q) for q in other],
        [(*at(back, s), other[0]) for s in (0, -1, 1, 2)],
    )


class Gather:
    def __init__(self, own, every, send_sem, recv_sem, me, side):
        self.own, self.every, self.send_sem, self.recv_sem = own, every, send_sem, recv_sem
        self.me, self.side, self.rows = me, side, own.shape[0]
        self.unit = self.rows // 4
        self.sent, self.pending = [], {}
        for link, (dx, dy) in enumerate(STEPS):
            flat = [p for stage in pieces_of(link) for p in stage]
            for k, (ox, oy, q) in enumerate(flat):
                key = self.key(ox - dx, oy - dy, q)
                assert key not in self.pending
                self.pending[key] = (link, k)
        self.arrival = dict(self.pending)

    def key(self, ox, oy, q):
        return ox % self.side, oy % self.side, q

    def start_row(self, ox, oy):
        x, y = (lax.rem(m + (o % self.side), self.side) for m, o in zip(self.me, (ox, oy)))
        return pl.multiple_of((x * self.side + y) * self.rows, self.unit)

    def place(self, ox, oy, q):
        return self.every.at[pl.ds(pl.multiple_of(self.start_row(ox, oy) + q * self.unit, 8), self.unit)]

    def copy(self, link, k, source, target):
        dx, dy = STEPS[link]
        x, y = (lax.rem(m + d + self.side, self.side) for m, d in zip(self.me, (dx, dy)))
        return pltpu.make_async_remote_copy(
            src_ref=source,
            dst_ref=target,
            send_sem=self.send_sem.at[link, k],
            recv_sem=self.recv_sem.at[link, k],
            device_id={"tp": x * self.side + y},
            device_id_type=MESH,
        )

    def wait(self, ox, oy, q):
        found = self.pending.pop(self.key(ox, oy, q), None)
        if found is not None:
            place = self.place(ox, oy, q)
            self.copy(*found, place, place).wait_recv()

    def send(self, stage, only=slice(None)):
        todo = [(link, pieces_of(link)) for link in range(4)]
        count = len(todo[0][1][stage])
        for i in range(count)[only]:
            for link, stages in todo:
                k = sum(len(s) for s in stages[:stage]) + i
                ox, oy, q = stages[stage][i]
                place = self.place(ox, oy, q)
                if (ox, oy) == (0, 0):
                    source = self.own.at[pl.ds(q * self.unit, self.unit)]
                else:
                    self.wait(ox, oy, q)
                    source = place
                self.copy(link, k, source, place).start()
                self.sent.append((link, k, place))

    def wait_shard(self, ox, oy):
        for q in range(4):
            self.wait(ox, oy, q)

    def finish(self):
        for key in list(self.pending):
            self.wait(*key)
        for link, k, place in self.sent:
            self.copy(link, k, place, place).wait_send()


def gather_kernel(
    side, x_ref, dy_ref, pre_ref, w_down_ref, w_in_ref,
    x_all, dy_all, hidden_ref, d_pre_ref, dx_ref,
    w_down, w_in, dy_buf, pre_buf, hidden_buf, d_pre_buf, dx_buf,
    x_send, x_recv, dy_send, dy_recv, load_sem, store_sem, weight_sem,
):
    rows, depth = dy_ref.shape
    width = pre_ref.shape[1]
    t = lax.axis_index("tp")
    me = lax.div(t, side), lax.rem(t, side)

    barrier = pltpu.get_barrier_semaphore()
    for dx, dy in STEPS:
        x, y = (lax.rem(m + d + side, side) for m, d in zip(me, (dx, dy)))
        pl.semaphore_signal(barrier, inc=1, device_id={"tp": x * side + y}, device_id_type=MESH)
    pl.semaphore_wait(barrier, 4)

    dys = Gather(dy_ref, dy_all, dy_send, dy_recv, me, side)
    xs = Gather(x_ref, x_all, x_send, x_recv, me, side)
    dys.send(0)
    loads = [
        pltpu.make_async_copy(w_down_ref, w_down, weight_sem.at[0]),
        pltpu.make_async_copy(w_in_ref, w_in, weight_sem.at[1]),
    ]
    for load in loads:
        load.start()

    def compute(ox, oy, own=None):
        x, y = lax.rem(me[0] + ox + side, side), lax.rem(me[1] + oy + side, side)
        here = pl.ds(pl.multiple_of((x * side + y) * rows, rows), rows)
        copies = [
            pltpu.make_async_copy(dy_all.at[here] if own is None else own, dy_buf, load_sem.at[0]),
            pltpu.make_async_copy(pre_ref.at[here], pre_buf, load_sem.at[1]),
        ]
        for c in copies:
            c.start()
        for c in copies:
            c.wait()

        @pl.loop(0, width // TILE)
        def _(n):
            tile = pl.ds(pl.multiple_of(n * TILE, TILE), TILE)
            d_hidden = lax.dot_general(
                dy_buf[...], w_down[tile, :], (((1,), (1,)), ((), ())), preferred_element_type=jnp.float32
            )
            hidden, back = jax.vjp(act, pre_buf[:, tile].astype(jnp.float32))
            hidden_buf[:, tile] = hidden.astype(hidden_buf.dtype)
            d_pre_buf[:, tile] = back(d_hidden)[0].astype(d_pre_buf.dtype)

        @pl.loop(0, depth // TILE)
        def _(n):
            tile = pl.ds(pl.multiple_of(n * TILE, TILE), TILE)
            dx_buf[:, tile] = lax.dot_general(
                d_pre_buf[...], w_in[tile, :], (((1,), (1,)), ((), ())), preferred_element_type=jnp.float32
            ).astype(dx_buf.dtype)

        copies = [
            pltpu.make_async_copy(hidden_buf, hidden_ref.at[here], store_sem.at[0]),
            pltpu.make_async_copy(d_pre_buf, d_pre_ref.at[here], store_sem.at[1]),
            pltpu.make_async_copy(dx_buf, dx_ref.at[here], store_sem.at[2]),
        ]
        if own is not None:
            copies.append(pltpu.make_async_copy(dy_buf, dy_all.at[here], store_sem.at[3]))
        for c in copies:
            c.start()
        for c in copies:
            c.wait()

    def compute_many(offsets, count):
        pl.loop(0, count)(lambda k: compute(*offsets(k)))

    for load in loads:
        load.wait()
    dys.send(1)
    compute(0, 0, dy_ref)
    dys.send(2)
    for ox, oy in STEPS:
        dys.wait_shard(ox, oy)
    compute_many(lambda k: ((1 - 2 * k), 0), 2)
    dys.send(3)
    compute_many(lambda k: (0, (1 - 2 * k)), 2)
    dys.send(4)
    xs.send(0)
    for ox, oy in ((1, 1), (1, -1), (-1, 1), (-1, -1)):
        dys.wait_shard(ox, oy)
    compute_many(lambda k: (1 - 2 * lax.rem(k, 2), 1 - 2 * lax.div(k, 2)), 4)
    for ox, oy in ((2, 0), (0, 2)):
        dys.wait_shard(ox, oy)
    compute_many(lambda k: (2 * k, 2 - 2 * k), 2)
    xs.send(1)
    xs.send(2)
    for ox, oy in ((2, 1), (2, -1), (1, 2), (-1, 2), (2, 2)):
        dys.wait_shard(ox, oy)
    compute_many(lambda k: (2, 1 - 2 * k), 2)
    compute_many(lambda k: (1 - 2 * k, 2), 2)
    xs.send(3)
    compute(2, 2)
    own = pltpu.make_async_copy(x_ref, dy_buf, load_sem.at[0])
    own.start()
    own.wait()
    own = pltpu.make_async_copy(dy_buf, x_all.at[pl.ds(pl.multiple_of(t * rows, rows), rows)], store_sem.at[3])
    own.start()
    own.wait()
    xs.send(4)
    dys.finish()
    xs.finish()


def gather_and_differentiate(x, dy, pre, w_down, w_in, group):
    side = math.isqrt(group)
    assert side == 4 and side * side == group
    rows, depth = dy.shape
    width = pre.shape[1]
    assert rows % 32 == 0 and width % TILE == 0 and depth % TILE == 0
    like = jax.ShapeDtypeStruct
    any_space = pl.BlockSpec(memory_space=pl.ANY)
    flops = 4 * group * rows * depth * width
    return pl.pallas_call(
        functools.partial(gather_kernel, side),
        out_shape=(
            like((group * rows, depth), x.dtype),
            like((group * rows, depth), x.dtype),
            like((group * rows, width), x.dtype),
            like((group * rows, width), x.dtype),
            like((group * rows, depth), x.dtype),
        ),
        in_specs=[any_space] * 5,
        out_specs=[any_space] * 5,
        scratch_shapes=[
            pltpu.VMEM((width, depth), x.dtype),
            pltpu.VMEM((depth, width), x.dtype),
            pltpu.VMEM((rows, depth), x.dtype),
            pltpu.VMEM((rows, width), x.dtype),
            pltpu.VMEM((rows, width), x.dtype),
            pltpu.VMEM((rows, width), x.dtype),
            pltpu.VMEM((rows, depth), x.dtype),
            pltpu.SemaphoreType.DMA((4, 15)),
            pltpu.SemaphoreType.DMA((4, 15)),
            pltpu.SemaphoreType.DMA((4, 15)),
            pltpu.SemaphoreType.DMA((4, 15)),
            pltpu.SemaphoreType.DMA((2,)),
            pltpu.SemaphoreType.DMA((4,)),
            pltpu.SemaphoreType.DMA((2,)),
        ],
        compiler_params=pltpu.CompilerParams(
            collective_id=0, has_side_effects=True, vmem_limit_bytes=67_043_328
        ),
        cost_estimate=pl.CostEstimate(flops=flops, bytes_accessed=2 * group * rows * (5 * depth + 3 * width), transcendentals=0),
        name="gather_and_differentiate",
    )(x, dy, pre, w_down, w_in)


def solution(mesh):
    group = mesh.shape["tp"]

    def step(x, dy, pre, w_in, w_down):
        x_all, dy_all, hidden, d_pre, dx = gather_and_differentiate(x, dy, pre, w_down, w_in, group)
        dx = lax.psum_scatter(dx, "tp", tiled=True)
        dw_down = tn_matmul(hidden, dy_all, 512, tile_b=True)
        return dx, tn_matmul(x_all, d_pre, 512), dw_down

    tokens = P(("dp", "tp"), None)
    return jax.shard_map(
        step,
        mesh=mesh,
        in_specs=(tokens, tokens, P("dp", "tp"), P(None, "tp"), P("tp", None)),
        out_specs=(tokens, P("dp", "tp"), tokens),
        check_vma=False,
    )
```

```python
import functools
import math

import jax
import jax.numpy as jnp
from jax import lax
from jax.experimental import pallas as pl
from jax.experimental.pallas import tpu as pltpu
from jax.sharding import PartitionSpec as P


MESH = pl.DeviceIdType.MESH
TILE = 256


def act(pre):
    return jax.nn.gelu(pre)


def dw_in_kernel(x_ref, d_pre_ref, dw_down_in, dw_in_ref, dw_down_ref, slab, load_sem, store_sem):
    step, steps = pl.program_id(0), pl.num_programs(0)
    height = slab.shape[1]
    slot = lax.rem(step, 2)

    def load(i, slot):
        rows = pl.ds(pl.multiple_of(i * height, height), height)
        return pltpu.make_async_copy(dw_down_in.at[rows], slab.at[slot], load_sem.at[slot])

    def store(i, slot):
        rows = pl.ds(pl.multiple_of(i * height, height), height)
        return pltpu.make_async_copy(slab.at[slot], dw_down_ref.at[rows], store_sem.at[slot])

    @pl.when(step >= 2)
    def _():
        store(step - 2, slot).wait()

    load(step, slot).start()
    dw_in_ref[...] = lax.dot_general(
        x_ref[...], d_pre_ref[...], (((0,), (0,)), ((), ())), preferred_element_type=jnp.float32
    ).astype(dw_in_ref.dtype)
    load(step, slot).wait()
    store(step, slot).start()

    @pl.when(step == steps - 1)
    def _():
        store(step - 1, 1 - slot).wait()
        store(step, slot).wait()


def dw_in_and_copy(x, d_pre, dw_down, tile):
    tokens, depth = x.shape
    width = d_pre.shape[1]
    steps = depth // tile
    height = dw_down.shape[0] // steps
    assert depth % tile == 0 and steps >= 2 and height * steps == dw_down.shape[0] and height % 16 == 0
    return pl.pallas_call(
        dw_in_kernel,
        grid=(steps,),
        in_specs=[
            pl.BlockSpec((tokens, tile), lambda i: (0, i)),
            pl.BlockSpec((tokens, width), lambda i: (0, 0)),
            pl.BlockSpec(memory_space=pl.ANY),
        ],
        out_specs=[pl.BlockSpec((tile, width), lambda i: (i, 0)), pl.BlockSpec(memory_space=pl.ANY)],
        out_shape=[jax.ShapeDtypeStruct((depth, width), x.dtype), jax.ShapeDtypeStruct(dw_down.shape, x.dtype)],
        scratch_shapes=[
            pltpu.VMEM((2, height, dw_down.shape[1]), x.dtype),
            pltpu.SemaphoreType.DMA((2,)),
            pltpu.SemaphoreType.DMA((2,)),
        ],
        compiler_params=pltpu.CompilerParams(vmem_limit_bytes=60 * 1024 * 1024),
        cost_estimate=pl.CostEstimate(
            flops=2 * tokens * depth * width,
            bytes_accessed=2 * (tokens * depth + tokens * width + 3 * depth * width),
            transcendentals=0,
        ),
    )(x, d_pre, dw_down)


STEPS = ((1, 0), (-1, 0), (0, 1), (0, -1))


def pieces_of(link):
    along_x, up = link < 2, link % 2 == 0
    mine = (0, 1) if along_x else (2, 3)
    other = (2, 3) if along_x else (0, 1)
    if not up:
        mine, other = mine[::-1], other[::-1]
    back = -1 if up else 1

    def at(first, second):
        return (first, second) if along_x else (second, first)

    return (
        [(*at(0, 0), q) for q in mine + other],
        [(*at(back, 0), mine[0])],
        [(*at(0, s), q) for s, order in ((-1, (0, 1)), (1, (1, 0))) for q in (min(other) + order[0], min(other) + order[1])],
        [(*at(0, 2), q) for q in other],
        [(*at(back, s), other[0]) for s in (0, -1, 1, 2)],
    )


class Gather:
    def __init__(self, own, every, send_sem, recv_sem, me, side):
        self.own, self.every, self.send_sem, self.recv_sem = own, every, send_sem, recv_sem
        self.me, self.side, self.rows = me, side, own.shape[0]
        self.unit = self.rows // 4
        self.sent, self.pending = [], {}
        for link, (dx, dy) in enumerate(STEPS):
            flat = [p for stage in pieces_of(link) for p in stage]
            for k, (ox, oy, q) in enumerate(flat):
                key = self.key(ox - dx, oy - dy, q)
                assert key not in self.pending
                self.pending[key] = (link, k)
        self.arrival = dict(self.pending)

    def key(self, ox, oy, q):
        return ox % self.side, oy % self.side, q

    def start_row(self, ox, oy):
        x, y = (lax.rem(m + (o % self.side), self.side) for m, o in zip(self.me, (ox, oy)))
        return pl.multiple_of((x * self.side + y) * self.rows, self.unit)

    def place(self, ox, oy, q):
        return self.every.at[pl.ds(pl.multiple_of(self.start_row(ox, oy) + q * self.unit, 8), self.unit)]

    def copy(self, link, k, source, target):
        dx, dy = STEPS[link]
        x, y = (lax.rem(m + d + self.side, self.side) for m, d in zip(self.me, (dx, dy)))
        return pltpu.make_async_remote_copy(
            src_ref=source,
            dst_ref=target,
            send_sem=self.send_sem.at[link, k],
            recv_sem=self.recv_sem.at[link, k],
            device_id={"tp": x * self.side + y},
            device_id_type=MESH,
        )

    def arriving(self, ox, oy, q):
        found = self.pending.pop(self.key(ox, oy, q), None)
        place = self.place(ox, oy, q)
        return [] if found is None else [self.copy(*found, place, place)]

    def wait(self, ox, oy, q):
        for c in self.arriving(ox, oy, q):
            c.wait_recv()

    def send(self, stage, only=slice(None)):
        for before, copy in self.forwards(stage, only):
            for c in before:
                c.wait_recv()
            copy.start()

    def forwards(self, stage, only=slice(None)):
        copies = []
        todo = [(link, pieces_of(link)) for link in range(4)]
        count = len(todo[0][1][stage])
        for i in range(count)[only]:
            for link, stages in todo:
                k = sum(len(s) for s in stages[:stage]) + i
                ox, oy, q = stages[stage][i]
                place = self.place(ox, oy, q)
                if (ox, oy) == (0, 0):
                    before, source = [], self.own.at[pl.ds(q * self.unit, self.unit)]
                else:
                    before, source = self.arriving(ox, oy, q), place
                copies.append((before, self.copy(link, k, source, place)))
                self.sent.append((link, k, place))
        return copies

    def wait_shard(self, ox, oy):
        for q in range(4):
            self.wait(ox, oy, q)

    def finish(self):
        for key in list(self.pending):
            self.wait(*key)
        for link, k, place in self.sent:
            self.copy(link, k, place, place).wait_send()


UP_DOWN = {"y": (2, 3), "x": (0, 1)}


def blocks_of(axis):
    up, down = UP_DOWN[axis]
    high, low = (0, 1) if axis == "y" else (2, 3)
    return {
        high: [(2, "relay", up), (1, "later", up), (-1, "direct", down), (0, "own", high)],
        low: [(2, "relay", down), (-1, "later", down), (1, "direct", up), (0, "own", low)],
    }


def barrier_with_neighbours(me, side):
    barrier = pltpu.get_barrier_semaphore()
    for dx, dy in STEPS:
        x, y = (lax.rem(m + d + side, side) for m, d in zip(me, (dx, dy)))
        pl.semaphore_signal(barrier, inc=1, device_id={"tp": x * side + y}, device_id_type=MESH)
    pl.semaphore_wait(barrier, len(STEPS))


def run(copies):
    for c in copies:
        c.start()
    for c in copies:
        c.wait()


def gather_kernel(side, x_ref, dy_ref, pre_ref, w_down_ref, w_in_ref, x_all, dy_all, hidden_ref, d_pre_ref, dw_down_ref, *rest):
    relay, direct, direct_last, later, own_terms = (rest[4 * i : 4 * i + 4] for i in range(5))
    (
        weights, stage, dy_buf, pre_buf, hidden_buf, d_pre, narrow, wide, dy_tile,
        x_send, x_recv, dy_send, dy_recv, load_sem, store_sem, stage_sem, block_sem, tile_sem, out_sem,
    ) = rest[20:]
    rows, depth = dy_ref.shape
    width = pre_ref.shape[1]
    quarter = depth // 4
    t = lax.axis_index("tp")
    me = lax.div(t, side), lax.rem(t, side)
    barrier_with_neighbours(me, side)

    dys = Gather(dy_ref, dy_all, dy_send, dy_recv, me, side)
    xs = Gather(x_ref, x_all, x_send, x_recv, me, side)
    dys.send(0)

    def load_quarter(q):
        return pltpu.make_async_copy(w_in_ref.at[pl.ds(q * quarter, quarter)], stage, stage_sem)

    def tile_at(n, size=TILE):
        return pl.ds(n * size if isinstance(n, int) else pl.multiple_of(n * size, size), size)

    load_quarter(0).start()

    @pl.loop(0, width // TILE)
    def _(n):
        run([pltpu.make_async_copy(w_down_ref.at[tile_at(n)], dy_buf.at[pl.ds(0, TILE)], load_sem.at[0])])
        for k in range(4):
            weights[k, :, tile_at(n)] = dy_buf[0:TILE, k * quarter : (k + 1) * quarter].T

    def rows_of(ox, oy):
        x, y = lax.rem(me[0] + ox + side, side), lax.rem(me[1] + oy + side, side)
        return pl.ds(pl.multiple_of((x * side + y) * rows, rows), rows)

    def wrap(offset):
        return offset % side if isinstance(offset, int) else lax.rem(offset + side, side)

    half = [pl.ds(0, rows), pl.ds(rows, rows)]
    stores = []

    def step_hidden(*pair, own=None):
        here = [rows_of(*offset) for offset in pair]
        at = [d_pre.at[wrap(ox), wrap(oy)] for ox, oy in pair]
        run(
            [
                pltpu.make_async_copy(dy_ref if i == own else dy_all.at[here[i]], dy_buf.at[half[i]], load_sem.at[i])
                for i in range(2)
            ]
            + [pltpu.make_async_copy(pre_ref.at[here[i]], pre_buf.at[half[i]], load_sem.at[2 + i]) for i in range(2)]
        )
        flush()

        @pl.loop(0, width // TILE)
        def _(n):
            tile = tile_at(n)
            d_hidden = jnp.dot(
                dy_buf[...], weights[:, :, tile].reshape(depth, TILE), preferred_element_type=jnp.float32
            )
            hidden, back = jax.vjp(act, pre_buf[:, tile].astype(jnp.float32))
            hidden_buf[:, tile] = hidden.astype(hidden_buf.dtype)
            grad = back(d_hidden)[0].astype(d_pre.dtype)
            for i in range(2):
                at[i][:, tile] = grad[i * rows : (i + 1) * rows]

        for i in range(2):
            stores.append(pltpu.make_async_copy(hidden_buf.at[half[i]], hidden_ref.at[here[i]], store_sem.at[i]))
            stores.append(pltpu.make_async_copy(at[i], d_pre_ref.at[here[i]], store_sem.at[2 + i]))
            if i == own:
                stores.append(pltpu.make_async_copy(dy_buf.at[half[i]], dy_all.at[here[i]], store_sem.at[4]))
        for c in stores:
            c.start()

    def flush():
        for c in stores:
            c.wait()
        stores.clear()

    def steps_hidden(pair):
        flush()

        @pl.loop(0, 2)
        def _(k):
            step_hidden(*pair(k))
            flush()

    leaving = {0: [], 1: []}

    def step_dx(axis, q, offset, kind, index):
        exact = kind in ("later", "own")
        buf, which = (wide, 0) if exact else (narrow, 1)
        for c in leaving[which]:
            c.wait()

        @pl.loop(0, quarter // TILE * 2)
        def _(n):
            tile = tile_at(lax.div(n, 2))
            two = pl.ds(lax.rem(n, 2) * (side // 2), side // 2)
            lines = d_pre[two, offset % side] if axis == "y" else d_pre[offset % side, two]
            term = jnp.dot(
                lines.reshape(side // 2 * rows, width), weights[q, :, tile], preferred_element_type=jnp.float32
            )
            buf[two, :, tile] = term.astype(buf.dtype).reshape(side // 2, rows, TILE)

        if kind == "direct":
            cut = [(buf.at[pl.ds(1, side - 1)], direct[index]), (buf.at[0], direct_last[index])]
        else:
            cut = [(buf, {"relay": relay, "later": later, "own": own_terms}[kind][index])]
        leaving[which] = [pltpu.make_async_copy(*c, block_sem.at[which, i]) for i, c in enumerate(cut)]
        for c in leaving[which]:
            c.start()

    dys.send(1)
    dys.send(2)
    for offset in STEPS:
        dys.wait_shard(*offset)
    steps_hidden(lambda k: ((1 - k, k), (k - 1, -k)))
    dys.send(3)
    dys.send(4, slice(0, 3))
    for s in (1, -1):
        for offset in ((1, s), (-1, s)):
            dys.wait_shard(*offset)
        step_hidden((1, s), (-1, s))
        if s == 1:
            dys.send(4, slice(3, 4))
            xs.send(0)
    for offset in ((2, 0), (0, 2)):
        dys.wait_shard(*offset)
    step_hidden((2, 0), (0, 2))
    for offset in ((2, 1), (2, -1), (1, 2), (-1, 2)):
        dys.wait_shard(*offset)
    steps_hidden(lambda k: ((2, 1 - 2 * k), (1 - 2 * k, 2)))
    dys.wait_shard(2, 2)
    step_hidden((0, 0), (2, 2), own=0)
    xs.send(1)
    xs.send(2)
    flush()
    own = dy_buf.at[half[0]]
    run([pltpu.make_async_copy(x_ref, own, load_sem.at[0])])
    stores.append(pltpu.make_async_copy(own, x_all.at[rows_of(0, 0)], store_sem.at[0]))
    stores[-1].start()
    tiles = dy_tile.shape[-1]

    def load_tile(n, slot):
        return pltpu.make_async_copy(dy_all.at[:, tile_at(n, tiles)], dy_tile.at[slot], tile_sem.at[slot])

    def store_tile(n, slot):
        return pltpu.make_async_copy(stage.at[:, tile_at(slot, tiles)], dw_down_ref.at[:, tile_at(n, tiles)], out_sem.at[slot])

    spare = side * side * rows - quarter
    hidden_loads = [
        pltpu.make_async_copy(hidden_ref.at[pl.ds(0, quarter)], weights.at[0], load_sem.at[1]),
        pltpu.make_async_copy(hidden_ref.at[pl.ds(quarter, spare)], weights.at[1, pl.ds(0, spare)], load_sem.at[2]),
    ]
    for axis in ("y", "x"):
        for q, blocks in blocks_of(axis).items():
            load_quarter(q).wait()

            @pl.loop(0, quarter // TILE)
            def _(n):
                weights[q, :, tile_at(n)] = stage[tile_at(n), :].T

            if q < 3:
                load_quarter(q + 1).start()
            else:
                for c in hidden_loads + [load_tile(0, 0)]:
                    c.start()
            for offset, kind, index in blocks:
                step_dx(axis, q, offset, kind, index)
            if q == 1:
                xs.send(3)
    xs.send(4, slice(0, 3))
    for c in hidden_loads:
        c.wait()
    count = depth // tiles
    final = xs.forwards(4, slice(3, 4))

    @pl.loop(0, count)
    def _(n):
        slot = lax.rem(n, 2)

        @pl.when(n == 4)
        def _():
            for before, copy in final:
                for c in before:
                    c.wait_recv()
                copy.start()

        @pl.when(n + 1 < count)
        def _():
            load_tile(n + 1, 1 - slot).start()

        @pl.when(n >= 2)
        def _():
            store_tile(n - 2, slot).wait()

        load_tile(n, slot).wait()
        hidden = jnp.concatenate([weights[0], weights[1, 0:spare, :]], axis=0)
        stage[:, tile_at(slot, tiles)] = lax.dot_general(
            hidden, dy_tile[slot], (((0,), (0,)), ((), ())), preferred_element_type=jnp.float32
        ).astype(stage.dtype)
        store_tile(n, slot).start()

    for c in stores + leaving[0] + leaving[1]:
        c.wait()
    for n in (count - 2, count - 1):
        store_tile(n, n % 2).wait()
    dys.finish()
    xs.finish()


def gather_and_differentiate(x, dy, pre, w_down, w_in, group):
    side = math.isqrt(group)
    assert side == 4 and side * side == group
    rows, depth = dy.shape
    width = pre.shape[1]
    quarter, tile = depth // 4, 2 * TILE
    assert rows % 32 == 0 and width % TILE == 0 and quarter % TILE == 0 and depth // tile > 4
    assert quarter < group * rows <= 2 * quarter and width == quarter
    like = jax.ShapeDtypeStruct
    any_space = pl.BlockSpec(memory_space=pl.ANY)
    block = (side, rows, quarter)
    dma = pltpu.SemaphoreType.DMA
    outs = pl.pallas_call(
        functools.partial(gather_kernel, side),
        out_shape=[like((group * rows, depth), x.dtype)] * 2
        + [like((group * rows, width), x.dtype)] * 2
        + [like((width, depth), x.dtype)]
        + [like(block, x.dtype)] * 4
        + [like((side - 1, *block[1:]), x.dtype)] * 4
        + [like(block[1:], x.dtype)] * 4
        + [like(block, jnp.float32)] * 8,
        in_specs=[any_space] * 5,
        out_specs=[any_space] * 25,
        scratch_shapes=[
            pltpu.VMEM((4, quarter, width), x.dtype),
            pltpu.VMEM((quarter, width), x.dtype),
            pltpu.VMEM((2 * rows, depth), x.dtype),
            pltpu.VMEM((2 * rows, width), x.dtype),
            pltpu.VMEM((2 * rows, width), x.dtype),
            pltpu.VMEM((side, side, rows, width), x.dtype),
            pltpu.VMEM(block, x.dtype),
            pltpu.VMEM(block, jnp.float32),
            pltpu.VMEM((2, group * rows, tile), x.dtype),
            *[dma((4, 15))] * 4,
            dma((4,)),
            dma((5,)),
            dma,
            dma((2, 2)),
            dma((2,)),
            dma((2,)),
        ],
        compiler_params=pltpu.CompilerParams(
            collective_id=0, has_side_effects=True, vmem_limit_bytes=67_043_328
        ),
        cost_estimate=pl.CostEstimate(
            flops=6 * group * rows * depth * width,
            bytes_accessed=2 * (group * rows * (7 * depth + 4 * width) + 3 * depth * width),
            transcendentals=0,
        ),
        name="gather_and_differentiate",
    )(x, dy, pre, w_down, w_in)
    return *outs[:5], *(outs[5 + 4 * i : 9 + 4 * i] for i in range(5))


def shift(value, link, side):
    dx, dy = STEPS[link]
    target = lambda x, y: (x + dx) % side * side + (y + dy) % side
    return lax.ppermute(value, "tp", [(x * side + y, target(x, y)) for x in range(side) for y in range(side)])


def scatter_kernel(side, *refs):
    relay, direct, direct_last, later, own_terms = (refs[4 * i : 4 * i + 4] for i in range(5))
    (
        dx_ref, later_got, last_got, cross_got, later_out, cross_out, exact_in, narrow_in, sums, dx_buf,
        later_send, later_recv, last_send, last_recv, cross_send, cross_recv, exact_sem, narrow_sem, dx_sem,
    ) = refs[20:]
    rows, quarter = dx_buf.shape[1:]
    t = lax.axis_index("tp")
    me = lax.div(t, side), lax.rem(t, side)
    barrier_with_neighbours(me, side)

    def remote(link, source, target, send_sem, recv_sem):
        dx, dy = STEPS[link]
        x, y = (lax.rem(m + d + side, side) for m, d in zip(me, (dx, dy)))
        return pltpu.make_async_remote_copy(
            src_ref=source,
            dst_ref=target,
            send_sem=send_sem,
            recv_sem=recv_sem,
            device_id={"tp": x * side + y},
            device_id_type=MESH,
        )

    last_copies = [
        remote(link, direct_last[link], last_got.at[link], last_send.at[link], last_recv.at[link]) for link in range(4)
    ]
    later_copies = {
        (link, j): remote(link, later_out.at[link, j], later_got.at[link, j], later_send.at[link, j], later_recv.at[link, j])
        for link in range(4)
        for j in range(side)
    }
    for c in last_copies:
        c.start()

    takes = {}
    for axis, other in (("y", "x"), ("x", "y")):
        (up, down), (cross_up, cross_down) = UP_DOWN[axis], UP_DOWN[other]
        high, low = (0, 1) if axis == "y" else (2, 3)
        takes[high] = up, down, cross_up, cross_down
        takes[low] = down, up, cross_down, cross_up
    step = lambda link: 1 if link in (0, 2) else side - 1
    cross_copies = {
        (q, k): remote(
            takes[q][3 if k == 1 else 2], cross_out.at[q, k], cross_got.at[q, k], cross_send.at[q, k], cross_recv.at[q, k]
        )
        for q in range(4)
        for k in range(3)
    }

    def add(target, *parts):
        strip = 16

        @pl.loop(0, rows // strip)
        def _(i):
            at = pl.ds(pl.multiple_of(i * strip, strip), strip)
            total = parts[0][at, :].astype(jnp.float32)
            for part in parts[1:]:
                total = total + part[at, :].astype(jnp.float32)
            target[at, :] = total.astype(target.dtype)

    order = [2, 1, side - 1, 0]
    tasks = [("later", link, j, later[link].at[j], relay[link].at[j]) for j in order for link in range(4)]
    for j in order:
        for q in range(4):
            link = takes[q][1]
            tasks.append(("sum", q, j, own_terms[q].at[j], None if j == 0 else direct[link].at[j - 1]))
    slots = exact_in.shape[0]

    def loads(n):
        _, _, _, exact, narrow = tasks[n]
        slot = n % slots
        copies = [pltpu.make_async_copy(exact, exact_in.at[slot], exact_sem.at[slot])]
        if narrow is not None:
            copies.append(pltpu.make_async_copy(narrow, narrow_in.at[slot], narrow_sem.at[slot]))
        return copies

    for n in range(slots - 1):
        for c in loads(n):
            c.start()
    for n, (kind, which, j, _, narrow) in enumerate(tasks):
        if n + slots - 1 < len(tasks):
            for c in loads(n + slots - 1):
                c.start()
        for c in loads(n):
            c.wait()
        exact, slot = exact_in.at[n % slots], n % slots
        if kind == "later":
            add(later_out.at[which, j], exact, narrow_in.at[slot])
            later_copies[which, j].start()
            continue
        q = which
        main, side_link, _, near_link = takes[q]
        later_copies[main, j].wait_recv()
        if narrow is None:
            last_copies[side_link].wait_recv()
            arrived = last_got.at[side_link]
        else:
            arrived = narrow_in.at[slot]
        parts = exact, later_got.at[main, j], arrived
        if j == 2:
            add(cross_out.at[q, 0], *parts)
            cross_copies[q, 0].start()
        elif j == step(near_link):
            add(cross_out.at[q, 1], *parts)
            cross_copies[q, 1].start()
        else:
            add(sums.at[q, 0 if j == 0 else 1], *parts)
    for q in range(4):
        cross_copies[q, 0].wait_recv()
        add(cross_out.at[q, 2], sums.at[q, 1], cross_got.at[q, 0])
        cross_copies[q, 2].start()
    outs = []
    for q in range(4):
        cross_copies[q, 1].wait_recv()
        cross_copies[q, 2].wait_recv()
        add(dx_buf.at[q], sums.at[q, 0], cross_got.at[q, 2], cross_got.at[q, 1])
        outs.append(pltpu.make_async_copy(dx_buf.at[q], dx_ref.at[:, pl.ds(q * quarter, quarter)], dx_sem.at[q]))
        outs[-1].start()
    for c in outs:
        c.wait()
    for c in [*last_copies, *later_copies.values(), *cross_copies.values()]:
        c.wait_send()


def finish_scatter(relay, direct, direct_last, later, own_terms):
    side, rows, quarter = relay[0].shape
    kind = relay[0].dtype
    any_space = pl.BlockSpec(memory_space=pl.ANY)
    dma = pltpu.SemaphoreType.DMA
    piece, slots = (rows, quarter), 4
    return pl.pallas_call(
        functools.partial(scatter_kernel, side),
        out_shape=jax.ShapeDtypeStruct((rows, 4 * quarter), kind),
        in_specs=[any_space] * 20,
        out_specs=any_space,
        scratch_shapes=[
            pltpu.VMEM((4, side, *piece), kind),
            pltpu.VMEM((4, *piece), kind),
            pltpu.VMEM((4, 3, *piece), kind),
            pltpu.VMEM((4, side, *piece), kind),
            pltpu.VMEM((4, 3, *piece), kind),
            pltpu.VMEM((slots, *piece), jnp.float32),
            pltpu.VMEM((slots, *piece), kind),
            pltpu.VMEM((4, 2, *piece), jnp.float32),
            pltpu.VMEM((4, *piece), kind),
            dma((4, side)),
            dma((4, side)),
            dma((4,)),
            dma((4,)),
            dma((4, 3)),
            dma((4, 3)),
            dma((slots,)),
            dma((slots,)),
            dma((4,)),
        ],
        compiler_params=pltpu.CompilerParams(
            collective_id=1, has_side_effects=True, vmem_limit_bytes=67_043_328
        ),
        cost_estimate=pl.CostEstimate(
            flops=8 * side * rows * quarter, bytes_accessed=60 * side * rows * quarter, transcendentals=0
        ),
        name="finish_scatter",
    )(*relay, *direct, *direct_last, *later, *own_terms)


def solution(mesh):
    group = mesh.shape["tp"]
    side = math.isqrt(group)

    def step(x, dy, pre, w_in, w_down):
        x_all, _, _, d_pre, dw_down, relay, direct, direct_last, later, own_terms = gather_and_differentiate(
            x, dy, pre, w_down, w_in, group
        )
        relay = [shift(block, link, side) for link, block in enumerate(relay)]
        direct = [shift(block, link, side) for link, block in enumerate(direct)]
        dw_in, dw_down = dw_in_and_copy(x_all, d_pre, dw_down, 2 * TILE)
        dw_in, dw_down, later = lax.optimization_barrier((dw_in, dw_down, later))
        dx = finish_scatter(relay, direct, direct_last, later, own_terms)
        return dx, dw_in, dw_down

    tokens = P(("dp", "tp"), None)
    step = jax.shard_map(
        step,
        mesh=mesh,
        in_specs=(tokens, tokens, P("dp", "tp"), P(None, "tp"), P("tp", None)),
        out_specs=(tokens, P("dp", "tp"), tokens),
        check_vma=False,
    )
    return step
```

```python
import functools
import math

import jax
import jax.numpy as jnp
from jax import lax
from jax.experimental import pallas as pl
from jax.experimental.pallas import tpu as pltpu
from jax.sharding import PartitionSpec as P


MESH = pl.DeviceIdType.MESH
TILE = 256


def act(pre):
    return jax.nn.gelu(pre)


def dw_in_kernel(x_ref, d_pre_ref, dw_down_in, dw_in_ref, dw_down_ref, slab, load_sem, store_sem):
    step, steps = pl.program_id(0), pl.num_programs(0)
    height = slab.shape[1]
    slot = lax.rem(step, 2)

    def load(i, slot):
        rows = pl.ds(pl.multiple_of(i * height, height), height)
        return pltpu.make_async_copy(dw_down_in.at[rows], slab.at[slot], load_sem.at[slot])

    def store(i, slot):
        rows = pl.ds(pl.multiple_of(i * height, height), height)
        return pltpu.make_async_copy(slab.at[slot], dw_down_ref.at[rows], store_sem.at[slot])

    @pl.when(step >= 2)
    def _():
        store(step - 2, slot).wait()

    load(step, slot).start()
    dw_in_ref[...] = lax.dot_general(
        x_ref[...], d_pre_ref[...], (((0,), (0,)), ((), ())), preferred_element_type=jnp.float32
    ).astype(dw_in_ref.dtype)
    load(step, slot).wait()
    store(step, slot).start()

    @pl.when(step == steps - 1)
    def _():
        store(step - 1, 1 - slot).wait()
        store(step, slot).wait()


def dw_in_and_copy(x, d_pre, dw_down, tile):
    tokens, depth = x.shape
    width = d_pre.shape[1]
    steps = depth // tile
    height = dw_down.shape[0] // steps
    assert depth % tile == 0 and steps >= 2 and height * steps == dw_down.shape[0] and height % 16 == 0
    return pl.pallas_call(
        dw_in_kernel,
        grid=(steps,),
        in_specs=[
            pl.BlockSpec((tokens, tile), lambda i: (0, i)),
            pl.BlockSpec((tokens, width), lambda i: (0, 0)),
            pl.BlockSpec(memory_space=pl.ANY),
        ],
        out_specs=[pl.BlockSpec((tile, width), lambda i: (i, 0)), pl.BlockSpec(memory_space=pl.ANY)],
        out_shape=[jax.ShapeDtypeStruct((depth, width), x.dtype), jax.ShapeDtypeStruct(dw_down.shape, x.dtype)],
        scratch_shapes=[
            pltpu.VMEM((2, height, dw_down.shape[1]), x.dtype),
            pltpu.SemaphoreType.DMA((2,)),
            pltpu.SemaphoreType.DMA((2,)),
        ],
        compiler_params=pltpu.CompilerParams(vmem_limit_bytes=60 * 1024 * 1024),
        cost_estimate=pl.CostEstimate(
            flops=2 * tokens * depth * width,
            bytes_accessed=2 * (tokens * depth + tokens * width + 3 * depth * width),
            transcendentals=0,
        ),
    )(x, d_pre, dw_down)


STEPS = ((1, 0), (-1, 0), (0, 1), (0, -1))


def pieces_of(link):
    along_x, up = link < 2, link % 2 == 0
    mine = (0, 1) if along_x else (2, 3)
    other = (2, 3) if along_x else (0, 1)
    if not up:
        mine, other = mine[::-1], other[::-1]
    back = -1 if up else 1

    def at(first, second):
        return (first, second) if along_x else (second, first)

    return (
        [(*at(0, 0), q) for q in mine + other],
        [(*at(back, 0), mine[0])],
        [(*at(0, s), q) for s, order in ((-1, (0, 1)), (1, (1, 0))) for q in (min(other) + order[0], min(other) + order[1])],
        [(*at(0, 2), q) for q in other],
        [(*at(back, s), other[0]) for s in (0, -1, 1, 2)],
    )


class Gather:
    def __init__(self, own, every, send_sem, recv_sem, me, side):
        self.own, self.every, self.send_sem, self.recv_sem = own, every, send_sem, recv_sem
        self.me, self.side, self.rows = me, side, own.shape[0]
        self.unit = self.rows // 4
        self.sent, self.pending = [], {}
        for link, (dx, dy) in enumerate(STEPS):
            flat = [p for stage in pieces_of(link) for p in stage]
            for k, (ox, oy, q) in enumerate(flat):
                key = self.key(ox - dx, oy - dy, q)
                assert key not in self.pending
                self.pending[key] = (link, k)
        self.arrival = dict(self.pending)

    def key(self, ox, oy, q):
        return ox % self.side, oy % self.side, q

    def start_row(self, ox, oy):
        x, y = (lax.rem(m + (o % self.side), self.side) for m, o in zip(self.me, (ox, oy)))
        return pl.multiple_of((x * self.side + y) * self.rows, self.unit)

    def place(self, ox, oy, q):
        return self.every.at[pl.ds(pl.multiple_of(self.start_row(ox, oy) + q * self.unit, 8), self.unit)]

    def copy(self, link, k, source, target):
        dx, dy = STEPS[link]
        x, y = (lax.rem(m + d + self.side, self.side) for m, d in zip(self.me, (dx, dy)))
        return pltpu.make_async_remote_copy(
            src_ref=source,
            dst_ref=target,
            send_sem=self.send_sem.at[link, k],
            recv_sem=self.recv_sem.at[link, k],
            device_id={"tp": x * self.side + y},
            device_id_type=MESH,
        )

    def arriving(self, ox, oy, q):
        found = self.pending.pop(self.key(ox, oy, q), None)
        place = self.place(ox, oy, q)
        return [] if found is None else [self.copy(*found, place, place)]

    def wait(self, ox, oy, q):
        for c in self.arriving(ox, oy, q):
            c.wait_recv()

    def send(self, stage, only=slice(None)):
        for before, copy in self.forwards(stage, only):
            for c in before:
                c.wait_recv()
            copy.start()

    def forwards(self, stage, only=slice(None)):
        copies = []
        todo = [(link, pieces_of(link)) for link in range(4)]
        count = len(todo[0][1][stage])
        for i in range(count)[only]:
            for link, stages in todo:
                k = sum(len(s) for s in stages[:stage]) + i
                ox, oy, q = stages[stage][i]
                place = self.place(ox, oy, q)
                if (ox, oy) == (0, 0):
                    before, source = [], self.own.at[pl.ds(q * self.unit, self.unit)]
                else:
                    before, source = self.arriving(ox, oy, q), place
                copies.append((before, self.copy(link, k, source, place)))
                self.sent.append((link, k, place))
        return copies

    def wait_shard(self, ox, oy):
        for q in range(4):
            self.wait(ox, oy, q)

    def finish(self):
        for key in list(self.pending):
            self.wait(*key)
        for link, k, place in self.sent:
            self.copy(link, k, place, place).wait_send()


UP_DOWN = {"y": (2, 3), "x": (0, 1)}


def blocks_of(axis):
    up, down = UP_DOWN[axis]
    high, low = (0, 1) if axis == "y" else (2, 3)
    return {
        high: [(2, "relay", up), (1, "later", up), (-1, "direct", down), (0, "own", high)],
        low: [(2, "relay", down), (-1, "later", down), (1, "direct", up), (0, "own", low)],
    }


def barrier_with_neighbours(me, side):
    barrier = pltpu.get_barrier_semaphore()
    for dx, dy in STEPS:
        x, y = (lax.rem(m + d + side, side) for m, d in zip(me, (dx, dy)))
        pl.semaphore_signal(barrier, inc=1, device_id={"tp": x * side + y}, device_id_type=MESH)
    pl.semaphore_wait(barrier, len(STEPS))


def run(copies):
    for c in copies:
        c.start()
    for c in copies:
        c.wait()


def gather_kernel(side, x_ref, dy_ref, pre_ref, w_down_ref, w_in_ref, x_all, dy_all, hidden_ref, d_pre_ref, dw_down_ref, *rest):
    relay, direct, direct_last, later, own_terms = (rest[4 * i : 4 * i + 4] for i in range(5))
    (
        weights, stage, dy_buf, pre_buf, hidden_buf, d_pre, narrow, wide, dy_tile,
        x_send, x_recv, dy_send, dy_recv, load_sem, store_sem, stage_sem, block_sem, tile_sem, out_sem,
    ) = rest[20:]
    rows, depth = dy_ref.shape
    width = pre_ref.shape[1]
    quarter = depth // 4
    t = lax.axis_index("tp")
    me = lax.div(t, side), lax.rem(t, side)
    barrier_with_neighbours(me, side)

    dys = Gather(dy_ref, dy_all, dy_send, dy_recv, me, side)
    xs = Gather(x_ref, x_all, x_send, x_recv, me, side)
    dys.send(0)

    def load_quarter(q):
        return pltpu.make_async_copy(w_in_ref.at[pl.ds(q * quarter, quarter)], stage, stage_sem)

    def tile_at(n, size=TILE):
        return pl.ds(n * size if isinstance(n, int) else pl.multiple_of(n * size, size), size)

    load_quarter(0).start()

    @pl.loop(0, width // TILE)
    def _(n):
        run([pltpu.make_async_copy(w_down_ref.at[tile_at(n)], dy_buf.at[pl.ds(0, TILE)], load_sem.at[0])])
        for k in range(4):
            weights[k, :, tile_at(n)] = dy_buf[0:TILE, k * quarter : (k + 1) * quarter].T

    def rows_of(ox, oy):
        x, y = lax.rem(me[0] + ox + side, side), lax.rem(me[1] + oy + side, side)
        return pl.ds(pl.multiple_of((x * side + y) * rows, rows), rows)

    def wrap(offset):
        return offset % side if isinstance(offset, int) else lax.rem(offset + side, side)

    half = [pl.ds(0, rows), pl.ds(rows, rows)]
    stores = []

    def step_hidden(*pair, own=None):
        here = [rows_of(*offset) for offset in pair]
        at = [d_pre.at[wrap(ox), wrap(oy)] for ox, oy in pair]
        count = range(len(pair))
        run(
            [
                pltpu.make_async_copy(dy_ref if i == own else dy_all.at[here[i]], dy_buf.at[half[i]], load_sem.at[i])
                for i in count
            ]
            + [pltpu.make_async_copy(pre_ref.at[here[i]], pre_buf.at[half[i]], load_sem.at[2 + i]) for i in count]
        )
        flush()
        used = slice(0, len(pair) * rows)

        @pl.loop(0, width // TILE)
        def _(n):
            tile = tile_at(n)
            d_hidden = jnp.dot(
                dy_buf[used, :], weights[:, :, tile].reshape(depth, TILE), preferred_element_type=jnp.float32
            )
            hidden, back = jax.vjp(act, pre_buf[used, tile].astype(jnp.float32))
            hidden_buf[used, tile] = hidden.astype(hidden_buf.dtype)
            grad = back(d_hidden)[0].astype(d_pre.dtype)
            for i in count:
                at[i][:, tile] = grad[i * rows : (i + 1) * rows]

        for i in count:
            stores.append(pltpu.make_async_copy(hidden_buf.at[half[i]], hidden_ref.at[here[i]], store_sem.at[i]))
            stores.append(pltpu.make_async_copy(at[i], d_pre_ref.at[here[i]], store_sem.at[2 + i]))
            if i == own:
                stores.append(pltpu.make_async_copy(dy_buf.at[half[i]], dy_all.at[here[i]], store_sem.at[4]))
        for c in stores:
            c.start()

    def flush():
        for c in stores:
            c.wait()
        stores.clear()

    def steps_hidden(pair):
        flush()

        @pl.loop(0, 2)
        def _(k):
            step_hidden(*pair(k))
            flush()

    leaving = {0: [], 1: []}

    def step_dx(axis, q, offset, kind, index):
        exact = kind in ("later", "own")
        buf, which = (wide, 0) if exact else (narrow, 1)
        for c in leaving[which]:
            c.wait()

        @pl.loop(0, quarter // TILE)
        def _(n):
            tile = tile_at(n)
            lines = d_pre[:, offset % side] if axis == "y" else d_pre[offset % side]
            term = jnp.dot(lines.reshape(side * rows, width), weights[q, :, tile], preferred_element_type=jnp.float32)
            buf[:, :, tile] = term.astype(buf.dtype).reshape(side, rows, TILE)

        if kind == "direct":
            cut = [(buf.at[pl.ds(1, side - 1)], direct[index]), (buf.at[0], direct_last[index])]
        else:
            cut = [(buf, {"relay": relay, "later": later, "own": own_terms}[kind][index])]
        leaving[which] = [pltpu.make_async_copy(*c, block_sem.at[which, i]) for i, c in enumerate(cut)]
        for c in leaving[which]:
            c.start()

    dys.send(1)
    dys.send(2)
    step_hidden((0, 0), own=0)
    for offset in STEPS:
        dys.wait_shard(*offset)
    steps_hidden(lambda k: ((1 - k, k), (k - 1, -k)))
    dys.send(3)
    dys.send(4, slice(0, 3))
    for s in (1, -1):
        for offset in ((1, s), (-1, s)):
            dys.wait_shard(*offset)
        step_hidden((1, s), (-1, s))
        if s == 1:
            dys.send(4, slice(3, 4))
            xs.send(0)
    for shards in (((2, 0), (0, 2)), ((2, -1), (-1, 2)), ((2, 1), (1, 2)), ((2, 2),)):
        for offset in shards:
            dys.wait_shard(*offset)
        step_hidden(*shards)
    flush()
    own = dy_buf.at[half[0]]
    run([pltpu.make_async_copy(x_ref, own, load_sem.at[0])])
    stores.append(pltpu.make_async_copy(own, x_all.at[rows_of(0, 0)], store_sem.at[0]))
    stores[-1].start()
    tiles = dy_tile.shape[-1]

    def load_tile(n, slot):
        return pltpu.make_async_copy(dy_all.at[:, tile_at(n, tiles)], dy_tile.at[slot], tile_sem.at[slot])

    def store_tile(n, slot):
        return pltpu.make_async_copy(stage.at[:, tile_at(slot, tiles)], dw_down_ref.at[:, tile_at(n, tiles)], out_sem.at[slot])

    spare = side * side * rows - quarter
    hidden_loads = [
        pltpu.make_async_copy(hidden_ref.at[pl.ds(0, quarter)], weights.at[0], load_sem.at[1]),
        pltpu.make_async_copy(hidden_ref.at[pl.ds(quarter, spare)], weights.at[1, pl.ds(0, spare)], load_sem.at[2]),
    ]
    for axis in ("y", "x"):
        for q, blocks in blocks_of(axis).items():
            load_quarter(q).wait()

            @pl.loop(0, quarter // TILE)
            def _(n):
                weights[q, :, tile_at(n)] = stage[tile_at(n), :].T

            if q < 3:
                load_quarter(q + 1).start()
            else:
                for c in hidden_loads + [load_tile(0, 0)]:
                    c.start()
            for offset, kind, index in blocks:
                step_dx(axis, q, offset, kind, index)
            if q == 0:
                xs.send(1)
                xs.send(2)
            if q == 2:
                xs.send(3)
    for c in hidden_loads:
        c.wait()
    count = depth // tiles
    forwards = {4: xs.forwards(4, slice(0, 3)), 7: xs.forwards(4, slice(3, 4))}

    @pl.loop(0, count)
    def _(n):
        slot = lax.rem(n, 2)

        for when, copies in forwards.items():

            @pl.when(n == when)
            def _():
                for before, copy in copies:
                    for c in before:
                        c.wait_recv()
                    copy.start()

        @pl.when(n + 1 < count)
        def _():
            load_tile(n + 1, 1 - slot).start()

        @pl.when(n >= 2)
        def _():
            store_tile(n - 2, slot).wait()

        load_tile(n, slot).wait()
        hidden = jnp.concatenate([weights[0], weights[1, 0:spare, :]], axis=0)
        stage[:, tile_at(slot, tiles)] = lax.dot_general(
            hidden, dy_tile[slot], (((0,), (0,)), ((), ())), preferred_element_type=jnp.float32
        ).astype(stage.dtype)
        store_tile(n, slot).start()

    for c in stores + leaving[0] + leaving[1]:
        c.wait()
    for n in (count - 2, count - 1):
        store_tile(n, n % 2).wait()
    dys.finish()
    xs.finish()


def gather_and_differentiate(x, dy, pre, w_down, w_in, group):
    side = math.isqrt(group)
    assert side == 4 and side * side == group
    rows, depth = dy.shape
    width = pre.shape[1]
    quarter, tile = depth // 4, 2 * TILE
    assert rows % 32 == 0 and width % TILE == 0 and quarter % TILE == 0 and depth // tile > 7
    assert quarter < group * rows <= 2 * quarter and width == quarter
    like = jax.ShapeDtypeStruct
    any_space = pl.BlockSpec(memory_space=pl.ANY)
    block = (side, rows, quarter)
    dma = pltpu.SemaphoreType.DMA
    outs = pl.pallas_call(
        functools.partial(gather_kernel, side),
        out_shape=[like((group * rows, depth), x.dtype)] * 2
        + [like((group * rows, width), x.dtype)] * 2
        + [like((width, depth), x.dtype)]
        + [like(block, x.dtype)] * 4
        + [like((side - 1, *block[1:]), x.dtype)] * 4
        + [like(block[1:], x.dtype)] * 4
        + [like(block, jnp.float32)] * 8,
        in_specs=[any_space] * 5,
        out_specs=[any_space] * 25,
        scratch_shapes=[
            pltpu.VMEM((4, quarter, width), x.dtype),
            pltpu.VMEM((quarter, width), x.dtype),
            pltpu.VMEM((2 * rows, depth), x.dtype),
            pltpu.VMEM((2 * rows, width), x.dtype),
            pltpu.VMEM((2 * rows, width), x.dtype),
            pltpu.VMEM((side, side, rows, width), x.dtype),
            pltpu.VMEM(block, x.dtype),
            pltpu.VMEM(block, jnp.float32),
            pltpu.VMEM((2, group * rows, tile), x.dtype),
            *[dma((4, 15))] * 4,
            dma((4,)),
            dma((5,)),
            dma,
            dma((2, 2)),
            dma((2,)),
            dma((2,)),
        ],
        compiler_params=pltpu.CompilerParams(
            collective_id=0, has_side_effects=True, vmem_limit_bytes=67_043_328
        ),
        cost_estimate=pl.CostEstimate(
            flops=6 * group * rows * depth * width,
            bytes_accessed=2 * (group * rows * (7 * depth + 4 * width) + 3 * depth * width),
            transcendentals=0,
        ),
        name="gather_and_differentiate",
    )(x, dy, pre, w_down, w_in)
    return *outs[:5], *(outs[5 + 4 * i : 9 + 4 * i] for i in range(5))


def shift(value, link, side):
    dx, dy = STEPS[link]
    target = lambda x, y: (x + dx) % side * side + (y + dy) % side
    return lax.ppermute(value, "tp", [(x * side + y, target(x, y)) for x in range(side) for y in range(side)])


def scatter_kernel(side, *refs):
    relay, direct, direct_last, later, own_terms = (refs[4 * i : 4 * i + 4] for i in range(5))
    (
        dx_ref, later_got, last_got, cross_got, later_out, cross_out, exact_in, narrow_in, sums, dx_buf,
        later_send, later_recv, last_send, last_recv, cross_send, cross_recv, exact_sem, narrow_sem, dx_sem,
    ) = refs[20:]
    rows, quarter = dx_buf.shape[1:]
    t = lax.axis_index("tp")
    me = lax.div(t, side), lax.rem(t, side)
    barrier_with_neighbours(me, side)

    def remote(link, source, target, send_sem, recv_sem):
        dx, dy = STEPS[link]
        x, y = (lax.rem(m + d + side, side) for m, d in zip(me, (dx, dy)))
        return pltpu.make_async_remote_copy(
            src_ref=source,
            dst_ref=target,
            send_sem=send_sem,
            recv_sem=recv_sem,
            device_id={"tp": x * side + y},
            device_id_type=MESH,
        )

    last_copies = [
        remote(link, direct_last[link], last_got.at[link], last_send.at[link], last_recv.at[link]) for link in range(4)
    ]
    later_copies = {
        (link, j): remote(link, later_out.at[link, j], later_got.at[link, j], later_send.at[link, j], later_recv.at[link, j])
        for link in range(4)
        for j in range(side)
    }
    for c in last_copies:
        c.start()

    takes = {}
    for axis, other in (("y", "x"), ("x", "y")):
        (up, down), (cross_up, cross_down) = UP_DOWN[axis], UP_DOWN[other]
        high, low = (0, 1) if axis == "y" else (2, 3)
        takes[high] = up, down, cross_up, cross_down
        takes[low] = down, up, cross_down, cross_up
    step = lambda link: 1 if link in (0, 2) else side - 1
    cross_copies = {
        (q, k): remote(
            takes[q][3 if k == 1 else 2], cross_out.at[q, k], cross_got.at[q, k], cross_send.at[q, k], cross_recv.at[q, k]
        )
        for q in range(4)
        for k in range(3)
    }

    def add(target, *parts):
        strip = 16

        @pl.loop(0, rows // strip)
        def _(i):
            at = pl.ds(pl.multiple_of(i * strip, strip), strip)
            total = parts[0][at, :].astype(jnp.float32)
            for part in parts[1:]:
                total = total + part[at, :].astype(jnp.float32)
            target[at, :] = total.astype(target.dtype)

    order = [2, 1, side - 1, 0]
    tasks = [("later", link, j, later[link].at[j], relay[link].at[j]) for j in order for link in range(4)]
    for j in order:
        for q in range(4):
            link = takes[q][1]
            tasks.append(("sum", q, j, own_terms[q].at[j], None if j == 0 else direct[link].at[j - 1]))
    slots = exact_in.shape[0]

    def loads(n):
        _, _, _, exact, narrow = tasks[n]
        slot = n % slots
        copies = [pltpu.make_async_copy(exact, exact_in.at[slot], exact_sem.at[slot])]
        if narrow is not None:
            copies.append(pltpu.make_async_copy(narrow, narrow_in.at[slot], narrow_sem.at[slot]))
        return copies

    for n in range(slots - 1):
        for c in loads(n):
            c.start()
    for n, (kind, which, j, _, narrow) in enumerate(tasks):
        if n + slots - 1 < len(tasks):
            for c in loads(n + slots - 1):
                c.start()
        for c in loads(n):
            c.wait()
        exact, slot = exact_in.at[n % slots], n % slots
        if kind == "later":
            add(later_out.at[which, j], exact, narrow_in.at[slot])
            later_copies[which, j].start()
            continue
        q = which
        main, side_link, _, near_link = takes[q]
        later_copies[main, j].wait_recv()
        if narrow is None:
            last_copies[side_link].wait_recv()
            arrived = last_got.at[side_link]
        else:
            arrived = narrow_in.at[slot]
        parts = exact, later_got.at[main, j], arrived
        if j == 2:
            add(cross_out.at[q, 0], *parts)
            cross_copies[q, 0].start()
        elif j == step(near_link):
            add(cross_out.at[q, 1], *parts)
            cross_copies[q, 1].start()
        else:
            add(sums.at[q, 0 if j == 0 else 1], *parts)
    for q in range(4):
        cross_copies[q, 0].wait_recv()
        add(cross_out.at[q, 2], sums.at[q, 1], cross_got.at[q, 0])
        cross_copies[q, 2].start()
    outs = []
    for q in range(4):
        cross_copies[q, 1].wait_recv()
        cross_copies[q, 2].wait_recv()
        add(dx_buf.at[q], sums.at[q, 0], cross_got.at[q, 2], cross_got.at[q, 1])
        outs.append(pltpu.make_async_copy(dx_buf.at[q], dx_ref.at[:, pl.ds(q * quarter, quarter)], dx_sem.at[q]))
        outs[-1].start()
    for c in outs:
        c.wait()
    for c in [*last_copies, *later_copies.values(), *cross_copies.values()]:
        c.wait_send()


def finish_scatter(relay, direct, direct_last, later, own_terms):
    side, rows, quarter = relay[0].shape
    kind = relay[0].dtype
    any_space = pl.BlockSpec(memory_space=pl.ANY)
    dma = pltpu.SemaphoreType.DMA
    piece, slots = (rows, quarter), 4
    return pl.pallas_call(
        functools.partial(scatter_kernel, side),
        out_shape=jax.ShapeDtypeStruct((rows, 4 * quarter), kind),
        in_specs=[any_space] * 20,
        out_specs=any_space,
        scratch_shapes=[
            pltpu.VMEM((4, side, *piece), kind),
            pltpu.VMEM((4, *piece), kind),
            pltpu.VMEM((4, 3, *piece), kind),
            pltpu.VMEM((4, side, *piece), kind),
            pltpu.VMEM((4, 3, *piece), kind),
            pltpu.VMEM((slots, *piece), jnp.float32),
            pltpu.VMEM((slots, *piece), kind),
            pltpu.VMEM((4, 2, *piece), jnp.float32),
            pltpu.VMEM((4, *piece), kind),
            dma((4, side)),
            dma((4, side)),
            dma((4,)),
            dma((4,)),
            dma((4, 3)),
            dma((4, 3)),
            dma((slots,)),
            dma((slots,)),
            dma((4,)),
        ],
        compiler_params=pltpu.CompilerParams(
            collective_id=1, has_side_effects=True, vmem_limit_bytes=67_043_328
        ),
        cost_estimate=pl.CostEstimate(
            flops=8 * side * rows * quarter, bytes_accessed=60 * side * rows * quarter, transcendentals=0
        ),
        name="finish_scatter",
    )(*relay, *direct, *direct_last, *later, *own_terms)


def solution(mesh):
    group = mesh.shape["tp"]
    side = math.isqrt(group)

    def step(x, dy, pre, w_in, w_down):
        x_all, _, _, d_pre, dw_down, relay, direct, direct_last, later, own_terms = gather_and_differentiate(
            x, dy, pre, w_down, w_in, group
        )
        relay = [shift(block, link, side) for link, block in enumerate(relay)]
        direct = [shift(block, link, side) for link, block in enumerate(direct)]
        dw_in, dw_down = dw_in_and_copy(x_all, d_pre, dw_down, 2 * TILE)
        dw_in, dw_down, later = lax.optimization_barrier((dw_in, dw_down, later))
        dx = finish_scatter(relay, direct, direct_last, later, own_terms)
        return dx, dw_in, dw_down

    tokens = P(("dp", "tp"), None)
    step = jax.shard_map(
        step,
        mesh=mesh,
        in_specs=(tokens, tokens, P("dp", "tp"), P(None, "tp"), P("tp", None)),
        out_specs=(tokens, P("dp", "tp"), tokens),
        check_vma=False,
    )
    return step
```

```python
import functools
import math

import jax
import jax.numpy as jnp
from jax import lax
from jax.experimental import pallas as pl
from jax.experimental.pallas import tpu as pltpu
from jax.sharding import PartitionSpec as P


MESH = pl.DeviceIdType.MESH
TILE = 256


def act(pre):
    return jax.nn.gelu(pre)


def dw_in_kernel(x_ref, d_pre_ref, dw_down_in, dw_in_ref, dw_down_ref, slab, load_sem, store_sem):
    step, steps = pl.program_id(0), pl.num_programs(0)
    height = slab.shape[1]
    slot = lax.rem(step, 2)

    def load(i, slot):
        rows = pl.ds(pl.multiple_of(i * height, height), height)
        return pltpu.make_async_copy(dw_down_in.at[rows], slab.at[slot], load_sem.at[slot])

    def store(i, slot):
        rows = pl.ds(pl.multiple_of(i * height, height), height)
        return pltpu.make_async_copy(slab.at[slot], dw_down_ref.at[rows], store_sem.at[slot])

    @pl.when(step >= 2)
    def _():
        store(step - 2, slot).wait()

    load(step, slot).start()
    dw_in_ref[...] = lax.dot_general(
        x_ref[...], d_pre_ref[...], (((0,), (0,)), ((), ())), preferred_element_type=jnp.float32
    ).astype(dw_in_ref.dtype)
    load(step, slot).wait()
    store(step, slot).start()

    @pl.when(step == steps - 1)
    def _():
        store(step - 1, 1 - slot).wait()
        store(step, slot).wait()


def dw_in_and_copy(x, d_pre, dw_down, tile):
    tokens, depth = x.shape
    width = d_pre.shape[1]
    steps = depth // tile
    height = dw_down.shape[0] // steps
    assert depth % tile == 0 and steps >= 2 and height * steps == dw_down.shape[0] and height % 16 == 0
    return pl.pallas_call(
        dw_in_kernel,
        grid=(steps,),
        in_specs=[
            pl.BlockSpec((tokens, tile), lambda i: (0, i)),
            pl.BlockSpec((tokens, width), lambda i: (0, 0)),
            pl.BlockSpec(memory_space=pl.ANY),
        ],
        out_specs=[pl.BlockSpec((tile, width), lambda i: (i, 0)), pl.BlockSpec(memory_space=pl.ANY)],
        out_shape=[jax.ShapeDtypeStruct((depth, width), x.dtype), jax.ShapeDtypeStruct(dw_down.shape, x.dtype)],
        scratch_shapes=[
            pltpu.VMEM((2, height, dw_down.shape[1]), x.dtype),
            pltpu.SemaphoreType.DMA((2,)),
            pltpu.SemaphoreType.DMA((2,)),
        ],
        compiler_params=pltpu.CompilerParams(vmem_limit_bytes=60 * 1024 * 1024),
        cost_estimate=pl.CostEstimate(
            flops=2 * tokens * depth * width,
            bytes_accessed=2 * (tokens * depth + tokens * width + 3 * depth * width),
            transcendentals=0,
        ),
    )(x, d_pre, dw_down)


STEPS = ((1, 0), (-1, 0), (0, 1), (0, -1))


def pieces_of(link):
    along_x, up = link < 2, link % 2 == 0
    mine = (0, 1) if along_x else (2, 3)
    other = (2, 3) if along_x else (0, 1)
    if not up:
        mine, other = mine[::-1], other[::-1]
    back = -1 if up else 1

    def at(first, second):
        return (first, second) if along_x else (second, first)

    return (
        [(*at(0, 0), q) for q in mine + other],
        [(*at(back, 0), mine[0])],
        [(*at(0, s), q) for s, order in ((-1, (0, 1)), (1, (1, 0))) for q in (min(other) + order[0], min(other) + order[1])],
        [(*at(0, 2), q) for q in other],
        [(*at(back, s), other[0]) for s in (0, -1, 1, 2)],
    )


class Gather:
    def __init__(self, own, every, send_sem, recv_sem, me, side):
        self.own, self.every, self.send_sem, self.recv_sem = own, every, send_sem, recv_sem
        self.me, self.side, self.rows = me, side, own.shape[0]
        self.unit = self.rows // 4
        self.sent, self.pending = [], {}
        for link, (dx, dy) in enumerate(STEPS):
            flat = [p for stage in pieces_of(link) for p in stage]
            for k, (ox, oy, q) in enumerate(flat):
                key = self.key(ox - dx, oy - dy, q)
                assert key not in self.pending
                self.pending[key] = (link, k)
        self.arrival = dict(self.pending)

    def key(self, ox, oy, q):
        return ox % self.side, oy % self.side, q

    def start_row(self, ox, oy):
        x, y = (lax.rem(m + (o % self.side), self.side) for m, o in zip(self.me, (ox, oy)))
        return pl.multiple_of((x * self.side + y) * self.rows, self.unit)

    def place(self, ox, oy, q):
        return self.every.at[pl.ds(pl.multiple_of(self.start_row(ox, oy) + q * self.unit, 8), self.unit)]

    def copy(self, link, k, source, target):
        dx, dy = STEPS[link]
        x, y = (lax.rem(m + d + self.side, self.side) for m, d in zip(self.me, (dx, dy)))
        return pltpu.make_async_remote_copy(
            src_ref=source,
            dst_ref=target,
            send_sem=self.send_sem.at[link, k],
            recv_sem=self.recv_sem.at[link, k],
            device_id={"tp": x * self.side + y},
            device_id_type=MESH,
        )

    def arriving(self, ox, oy, q):
        found = self.pending.pop(self.key(ox, oy, q), None)
        place = self.place(ox, oy, q)
        return [] if found is None else [self.copy(*found, place, place)]

    def wait(self, ox, oy, q):
        for c in self.arriving(ox, oy, q):
            c.wait_recv()

    def send(self, stage, only=slice(None)):
        for before, copy in self.forwards(stage, only):
            for c in before:
                c.wait_recv()
            copy.start()

    def forwards(self, stage, only=slice(None)):
        copies = []
        todo = [(link, pieces_of(link)) for link in range(4)]
        count = len(todo[0][1][stage])
        for i in range(count)[only]:
            for link, stages in todo:
                k = sum(len(s) for s in stages[:stage]) + i
                ox, oy, q = stages[stage][i]
                place = self.place(ox, oy, q)
                if (ox, oy) == (0, 0):
                    before, source = [], self.own.at[pl.ds(q * self.unit, self.unit)]
                else:
                    before, source = self.arriving(ox, oy, q), place
                copies.append((before, self.copy(link, k, source, place)))
                self.sent.append((link, k, place))
        return copies

    def wait_shard(self, ox, oy):
        for q in range(4):
            self.wait(ox, oy, q)

    def finish(self):
        for key in list(self.pending):
            self.wait(*key)
        for link, k, place in self.sent:
            self.copy(link, k, place, place).wait_send()


UP_DOWN = {"y": (2, 3), "x": (0, 1)}


def blocks_of(axis):
    up, down = UP_DOWN[axis]
    high, low = (0, 1) if axis == "y" else (2, 3)
    return {
        high: [(2, "relay", up), (1, "later", up), (-1, "direct", down), (0, "own", high)],
        low: [(2, "relay", down), (-1, "later", down), (1, "direct", up), (0, "own", low)],
    }


def barrier_with_neighbours(me, side):
    barrier = pltpu.get_barrier_semaphore()
    for dx, dy in STEPS:
        x, y = (lax.rem(m + d + side, side) for m, d in zip(me, (dx, dy)))
        pl.semaphore_signal(barrier, inc=1, device_id={"tp": x * side + y}, device_id_type=MESH)
    pl.semaphore_wait(barrier, len(STEPS))


def run(copies):
    for c in copies:
        c.start()
    for c in copies:
        c.wait()


def gather_kernel(side, x_ref, dy_ref, pre_ref, w_down_ref, w_in_ref, x_all, dy_all, hidden_ref, d_pre_ref, dw_down_ref, *rest):
    relay, direct, direct_last, later, own_terms = (rest[4 * i : 4 * i + 4] for i in range(5))
    (
        weights, stage, dy_buf, pre_buf, hidden_buf, d_pre, narrow, wide, dy_tile,
        x_send, x_recv, dy_send, dy_recv, load_sem, store_sem, stage_sem, block_sem, tile_sem, out_sem,
    ) = rest[20:]
    rows, depth = dy_ref.shape
    width = pre_ref.shape[1]
    quarter = depth // 4
    t = lax.axis_index("tp")
    me = lax.div(t, side), lax.rem(t, side)
    barrier_with_neighbours(me, side)

    dys = Gather(dy_ref, dy_all, dy_send, dy_recv, me, side)
    xs = Gather(x_ref, x_all, x_send, x_recv, me, side)
    dys.send(0)

    def load_quarter(q):
        return pltpu.make_async_copy(w_in_ref.at[pl.ds(q * quarter, quarter)], stage, stage_sem)

    def tile_at(n, size=TILE):
        return pl.ds(n * size if isinstance(n, int) else pl.multiple_of(n * size, size), size)

    load_quarter(0).start()

    @pl.loop(0, width // TILE)
    def _(n):
        run([pltpu.make_async_copy(w_down_ref.at[tile_at(n)], dy_buf.at[pl.ds(0, TILE)], load_sem.at[0])])
        for k in range(4):
            weights[k, :, tile_at(n)] = dy_buf[0:TILE, k * quarter : (k + 1) * quarter].T

    def rows_of(ox, oy):
        x, y = lax.rem(me[0] + ox + side, side), lax.rem(me[1] + oy + side, side)
        return pl.ds(pl.multiple_of((x * side + y) * rows, rows), rows)

    def wrap(offset):
        return offset % side if isinstance(offset, int) else lax.rem(offset + side, side)

    half = [pl.ds(0, rows), pl.ds(rows, rows)]
    stores = []

    def step_hidden(*pair, own=None):
        here = [rows_of(*offset) for offset in pair]
        at = [d_pre.at[wrap(ox), wrap(oy)] for ox, oy in pair]
        count = range(len(pair))
        run(
            [
                pltpu.make_async_copy(dy_ref if i == own else dy_all.at[here[i]], dy_buf.at[half[i]], load_sem.at[i])
                for i in count
            ]
            + [pltpu.make_async_copy(pre_ref.at[here[i]], pre_buf.at[half[i]], load_sem.at[2 + i]) for i in count]
        )
        flush()
        used = slice(0, len(pair) * rows)

        @pl.loop(0, width // TILE)
        def _(n):
            tile = tile_at(n)
            d_hidden = jnp.dot(
                dy_buf[used, :], weights[:, :, tile].reshape(depth, TILE), preferred_element_type=jnp.float32
            )
            hidden, back = jax.vjp(act, pre_buf[used, tile].astype(jnp.float32))
            hidden_buf[used, tile] = hidden.astype(hidden_buf.dtype)
            grad = back(d_hidden)[0].astype(d_pre.dtype)
            for i in count:
                at[i][:, tile] = grad[i * rows : (i + 1) * rows]

        for i in count:
            stores.append(pltpu.make_async_copy(hidden_buf.at[half[i]], hidden_ref.at[here[i]], store_sem.at[i]))
            stores.append(pltpu.make_async_copy(at[i], d_pre_ref.at[here[i]], store_sem.at[2 + i]))
            if i == own:
                stores.append(pltpu.make_async_copy(dy_buf.at[half[i]], dy_all.at[here[i]], store_sem.at[4]))
        for c in stores:
            c.start()

    def flush():
        for c in stores:
            c.wait()
        stores.clear()

    def steps_hidden(pair):
        flush()

        @pl.loop(0, 2)
        def _(k):
            step_hidden(*pair(k))
            flush()

    leaving = {0: [], 1: []}

    def step_dx(axis, q, offset, kind, index):
        exact = kind in ("later", "own")
        buf, which = (wide, 0) if exact else (narrow, 1)
        for c in leaving[which]:
            c.wait()

        @pl.loop(0, quarter // TILE)
        def _(n):
            tile = tile_at(n)
            lines = d_pre[:, offset % side] if axis == "y" else d_pre[offset % side]
            term = jnp.dot(lines.reshape(side * rows, width), weights[q, :, tile], preferred_element_type=jnp.float32)
            buf[:, :, tile] = term.astype(buf.dtype).reshape(side, rows, TILE)

        if kind == "direct":
            cut = [(buf.at[pl.ds(1, side - 1)], direct[index]), (buf.at[0], direct_last[index])]
        else:
            cut = [(buf, {"relay": relay, "later": later, "own": own_terms}[kind][index])]
        leaving[which] = [pltpu.make_async_copy(*c, block_sem.at[which, i]) for i, c in enumerate(cut)]
        for c in leaving[which]:
            c.start()

    dys.send(1)
    dys.send(2)
    step_hidden((0, 0), own=0)
    for offset in STEPS:
        dys.wait_shard(*offset)
    steps_hidden(lambda k: ((1 - k, k), (k - 1, -k)))
    dys.send(3)
    dys.send(4, slice(0, 3))
    for s in (1, -1):
        for offset in ((1, s), (-1, s)):
            dys.wait_shard(*offset)
        step_hidden((1, s), (-1, s))
        if s == 1:
            dys.send(4, slice(3, 4))
            xs.send(0)
    for shards in (((2, 0), (0, 2)), ((2, -1), (-1, 2)), ((2, 1), (1, 2)), ((2, 2),)):
        for offset in shards:
            dys.wait_shard(*offset)
        step_hidden(*shards)
    flush()
    own = dy_buf.at[half[0]]
    run([pltpu.make_async_copy(x_ref, own, load_sem.at[0])])
    stores.append(pltpu.make_async_copy(own, x_all.at[rows_of(0, 0)], store_sem.at[0]))
    stores[-1].start()
    tiles = dy_tile.shape[-1]

    def load_tile(n, slot):
        return pltpu.make_async_copy(dy_all.at[:, tile_at(n, tiles)], dy_tile.at[slot], tile_sem.at[slot])

    def store_tile(n, slot):
        return pltpu.make_async_copy(stage.at[:, tile_at(slot, tiles)], dw_down_ref.at[:, tile_at(n, tiles)], out_sem.at[slot])

    spare = side * side * rows - quarter
    hidden_loads = [
        pltpu.make_async_copy(hidden_ref.at[pl.ds(0, quarter)], weights.at[0], load_sem.at[1]),
        pltpu.make_async_copy(hidden_ref.at[pl.ds(quarter, spare)], weights.at[1, pl.ds(0, spare)], load_sem.at[2]),
    ]
    for axis in ("y", "x"):
        for q, blocks in blocks_of(axis).items():
            load_quarter(q).wait()

            @pl.loop(0, quarter // TILE)
            def _(n):
                weights[q, :, tile_at(n)] = stage[tile_at(n), :].T

            if q < 3:
                load_quarter(q + 1).start()
            else:
                for c in hidden_loads + [load_tile(0, 0)]:
                    c.start()
            for offset, kind, index in blocks:
                step_dx(axis, q, offset, kind, index)
            if q == 0:
                xs.send(1)
                xs.send(2)
            if q == 2:
                xs.send(3)
    for c in hidden_loads:
        c.wait()
    count = depth // tiles
    forwards = {4: xs.forwards(4, slice(0, 3)), 7: xs.forwards(4, slice(3, 4))}

    @pl.loop(0, count)
    def _(n):
        slot = lax.rem(n, 2)

        for when, copies in forwards.items():

            @pl.when(n == when)
            def _():
                for before, copy in copies:
                    for c in before:
                        c.wait_recv()
                    copy.start()

        @pl.when(n + 1 < count)
        def _():
            load_tile(n + 1, 1 - slot).start()

        @pl.when(n >= 2)
        def _():
            store_tile(n - 2, slot).wait()

        load_tile(n, slot).wait()
        hidden = jnp.concatenate([weights[0], weights[1, 0:spare, :]], axis=0)
        stage[:, tile_at(slot, tiles)] = lax.dot_general(
            hidden, dy_tile[slot], (((0,), (0,)), ((), ())), preferred_element_type=jnp.float32
        ).astype(stage.dtype)
        store_tile(n, slot).start()

    for c in stores + leaving[0] + leaving[1]:
        c.wait()
    for n in (count - 2, count - 1):
        store_tile(n, n % 2).wait()
    dys.finish()
    xs.finish()


def gather_and_differentiate(x, dy, pre, w_down, w_in, group):
    side = math.isqrt(group)
    assert side == 4 and side * side == group
    rows, depth = dy.shape
    width = pre.shape[1]
    quarter, tile = depth // 4, 2 * TILE
    assert rows % 32 == 0 and width % TILE == 0 and quarter % TILE == 0 and depth // tile > 7
    assert quarter < group * rows <= 2 * quarter and width == quarter
    like = jax.ShapeDtypeStruct
    any_space = pl.BlockSpec(memory_space=pl.ANY)
    block = (side, rows, quarter)
    dma = pltpu.SemaphoreType.DMA
    outs = pl.pallas_call(
        functools.partial(gather_kernel, side),
        out_shape=[like((group * rows, depth), x.dtype)] * 2
        + [like((group * rows, width), x.dtype)] * 2
        + [like((width, depth), x.dtype)]
        + [like(block, x.dtype)] * 4
        + [like((side - 1, *block[1:]), x.dtype)] * 4
        + [like(block[1:], x.dtype)] * 4
        + [like(block, jnp.float32)] * 8,
        in_specs=[any_space] * 5,
        out_specs=[any_space] * 25,
        scratch_shapes=[
            pltpu.VMEM((4, quarter, width), x.dtype),
            pltpu.VMEM((quarter, width), x.dtype),
            pltpu.VMEM((2 * rows, depth), x.dtype),
            pltpu.VMEM((2 * rows, width), x.dtype),
            pltpu.VMEM((2 * rows, width), x.dtype),
            pltpu.VMEM((side, side, rows, width), x.dtype),
            pltpu.VMEM(block, x.dtype),
            pltpu.VMEM(block, jnp.float32),
            pltpu.VMEM((2, group * rows, tile), x.dtype),
            *[dma((4, 15))] * 4,
            dma((4,)),
            dma((5,)),
            dma,
            dma((2, 2)),
            dma((2,)),
            dma((2,)),
        ],
        compiler_params=pltpu.CompilerParams(
            collective_id=0, has_side_effects=True, vmem_limit_bytes=67_043_328
        ),
        cost_estimate=pl.CostEstimate(
            flops=6 * group * rows * depth * width,
            bytes_accessed=2 * (group * rows * (7 * depth + 4 * width) + 3 * depth * width),
            transcendentals=0,
        ),
        name="gather_and_differentiate",
    )(x, dy, pre, w_down, w_in)
    return *outs[:5], *(outs[5 + 4 * i : 9 + 4 * i] for i in range(5))


def shift(value, link, side):
    dx, dy = STEPS[link]
    target = lambda x, y: (x + dx) % side * side + (y + dy) % side
    return lax.ppermute(value, "tp", [(x * side + y, target(x, y)) for x in range(side) for y in range(side)])


def links_of_quarters():
    takes = {}
    for axis, other in (("y", "x"), ("x", "y")):
        (up, down), (cross_up, cross_down) = UP_DOWN[axis], UP_DOWN[other]
        high, low = (0, 1) if axis == "y" else (2, 3)
        takes[high] = up, down, cross_up, cross_down
        takes[low] = down, up, cross_down, cross_up
    return takes


def scatter_kernel(side, *refs):
    relay, direct, later, own_terms = (refs[4 * i : 4 * i + 4] for i in range(4))
    (
        kept_ref, last_ref, later_got, cross_got, later_out, cross_out, exact_in, narrow_in, sums,
        later_send, later_recv, cross_send, cross_recv, exact_sem, narrow_sem, kept_sem,
    ) = refs[16:]
    rows, quarter = exact_in.shape[1:]
    t = lax.axis_index("tp")
    me = lax.div(t, side), lax.rem(t, side)
    barrier_with_neighbours(me, side)

    def remote(link, source, target, send_sem, recv_sem):
        dx, dy = STEPS[link]
        x, y = (lax.rem(m + d + side, side) for m, d in zip(me, (dx, dy)))
        return pltpu.make_async_remote_copy(
            src_ref=source,
            dst_ref=target,
            send_sem=send_sem,
            recv_sem=recv_sem,
            device_id={"tp": x * side + y},
            device_id_type=MESH,
        )

    later_copies = {
        (link, j): remote(link, later_out.at[link, j], later_got.at[link, j], later_send.at[link, j], later_recv.at[link, j])
        for link in range(4)
        for j in range(side)
    }
    takes = links_of_quarters()
    step = lambda link: 1 if link in (0, 2) else side - 1
    columns = [pl.ds(q * quarter, quarter) for q in range(4)]
    cross_copies = {
        (q, k): remote(
            takes[q][3 if k == 1 else 2],
            cross_out.at[q, k],
            last_ref.at[:, columns[q]] if k == 2 else cross_got.at[q, k],
            cross_send.at[q, k],
            cross_recv.at[q, k],
        )
        for q in range(4)
        for k in range(3)
    }

    def add(target, *parts):
        strip = 16

        @pl.loop(0, rows // strip)
        def _(i):
            at = pl.ds(pl.multiple_of(i * strip, strip), strip)
            total = parts[0][at, :].astype(jnp.float32)
            for part in parts[1:]:
                total = total + part[at, :].astype(jnp.float32)
            target[at, :] = total.astype(target.dtype)

    order = [2, 1, side - 1, 0]
    tasks = [("later", link, j, later[link].at[j], relay[link].at[j]) for j in order for link in range(4)]
    for j in order:
        for q in range(4):
            link = takes[q][1]
            tasks.append(("sum", q, j, own_terms[q].at[j], None if j == 0 else direct[link].at[j - 1]))
    slots = exact_in.shape[0]

    def loads(n):
        _, _, _, exact, narrow = tasks[n]
        slot = n % slots
        copies = [pltpu.make_async_copy(exact, exact_in.at[slot], exact_sem.at[slot])]
        if narrow is not None:
            copies.append(pltpu.make_async_copy(narrow, narrow_in.at[slot], narrow_sem.at[slot]))
        return copies

    for n in range(slots - 1):
        for c in loads(n):
            c.start()
    for n, (kind, which, j, _, narrow) in enumerate(tasks):
        if n + slots - 1 < len(tasks):
            for c in loads(n + slots - 1):
                c.start()
        for c in loads(n):
            c.wait()
        exact, slot = exact_in.at[n % slots], n % slots
        if kind == "later":
            add(later_out.at[which, j], exact, narrow_in.at[slot])
            later_copies[which, j].start()
            continue
        q = which
        main, _, _, near_link = takes[q]
        later_copies[main, j].wait_recv()
        parts = [exact, later_got.at[main, j]]
        if narrow is not None:
            parts.append(narrow_in.at[slot])
        if j == 2:
            add(cross_out.at[q, 0], *parts)
            cross_copies[q, 0].start()
        elif j == step(near_link):
            add(cross_out.at[q, 1], *parts)
            cross_copies[q, 1].start()
        else:
            add(sums.at[q, 0 if j == 0 else 1], *parts)
    for q in range(4):
        cross_copies[q, 0].wait_recv()
        add(cross_out.at[q, 2], sums.at[q, 1], cross_got.at[q, 0])
        cross_copies[q, 2].start()
    outs = []
    for q in range(4):
        cross_copies[q, 1].wait_recv()
        add(sums.at[q, 1], sums.at[q, 0], cross_got.at[q, 1])
        outs.append(pltpu.make_async_copy(sums.at[q, 1], kept_ref.at[:, columns[q]], kept_sem.at[q]))
        outs[-1].start()
    for c in outs:
        c.wait()
    for q in range(4):
        cross_copies[q, 2].wait_recv()
    for c in [*later_copies.values(), *cross_copies.values()]:
        c.wait_send()


def sum_and_scatter(relay, direct, later, own_terms):
    side, rows, quarter = relay[0].shape
    kind = relay[0].dtype
    any_space = pl.BlockSpec(memory_space=pl.ANY)
    dma = pltpu.SemaphoreType.DMA
    piece, slots = (rows, quarter), 4
    return pl.pallas_call(
        functools.partial(scatter_kernel, side),
        out_shape=[jax.ShapeDtypeStruct((rows, 4 * quarter), t) for t in (jnp.float32, kind)],
        in_specs=[any_space] * 16,
        out_specs=[any_space] * 2,
        scratch_shapes=[
            pltpu.VMEM((4, side, *piece), kind),
            pltpu.VMEM((4, 2, *piece), kind),
            pltpu.VMEM((4, side, *piece), kind),
            pltpu.VMEM((4, 3, *piece), kind),
            pltpu.VMEM((slots, *piece), jnp.float32),
            pltpu.VMEM((slots, *piece), kind),
            pltpu.VMEM((4, 2, *piece), jnp.float32),
            dma((4, side)),
            dma((4, side)),
            dma((4, 3)),
            dma((4, 3)),
            dma((slots,)),
            dma((slots,)),
            dma((4,)),
        ],
        compiler_params=pltpu.CompilerParams(
            collective_id=1, has_side_effects=True, vmem_limit_bytes=67_043_328
        ),
        cost_estimate=pl.CostEstimate(
            flops=8 * side * rows * quarter, bytes_accessed=60 * side * rows * quarter, transcendentals=0
        ),
        name="sum_and_scatter",
    )(*relay, *direct, *later, *own_terms)


def finish_kernel(kept_ref, last_ref, *refs):
    dx_ref = refs[-1]
    for q, direct in enumerate(refs[:-1]):

        @pl.when(pl.program_id(0) == q)
        def _():
            total = kept_ref[...] + direct[...].astype(jnp.float32) + last_ref[...].astype(jnp.float32)
            dx_ref[...] = total.astype(dx_ref.dtype)


def finish_dx(kept, last, direct_last):
    rows, depth = kept.shape
    piece = (rows, depth // 4)
    column = pl.BlockSpec(piece, lambda q: (0, q))
    takes = links_of_quarters()
    return pl.pallas_call(
        finish_kernel,
        grid=(4,),
        in_specs=[column, column] + [pl.BlockSpec(piece, lambda q: (0, 0))] * 4,
        out_specs=column,
        out_shape=jax.ShapeDtypeStruct(kept.shape, last.dtype),
        cost_estimate=pl.CostEstimate(flops=2 * rows * depth, bytes_accessed=10 * rows * depth, transcendentals=0),
        name="finish_dx",
    )(kept, last, *(direct_last[takes[q][1]] for q in range(4)))


def solution(mesh):
    group = mesh.shape["tp"]
    side = math.isqrt(group)

    def step(x, dy, pre, w_in, w_down):
        x_all, _, _, d_pre, dw_down, relay, direct, direct_last, later, own_terms = gather_and_differentiate(
            x, dy, pre, w_down, w_in, group
        )
        relay = [shift(block, link, side) for link, block in enumerate(relay)]
        direct = [shift(block, link, side) for link, block in enumerate(direct)]
        direct_last = [shift(block, link, side) for link, block in enumerate(direct_last)]
        dw_in, dw_down = dw_in_and_copy(x_all, d_pre, dw_down, 2 * TILE)
        dw_in, dw_down, later = lax.optimization_barrier((dw_in, dw_down, later))
        dx = finish_dx(*sum_and_scatter(relay, direct, later, own_terms), direct_last)
        return dx, dw_in, dw_down

    tokens = P(("dp", "tp"), None)
    step = jax.shard_map(
        step,
        mesh=mesh,
        in_specs=(tokens, tokens, P("dp", "tp"), P(None, "tp"), P("tp", None)),
        out_specs=(tokens, P("dp", "tp"), tokens),
        check_vma=False,
    )
    return step
```

```python
import functools
import math

import jax
import jax.numpy as jnp
from jax import lax
from jax.experimental import pallas as pl
from jax.experimental.pallas import tpu as pltpu
from jax.sharding import PartitionSpec as P


MESH = pl.DeviceIdType.MESH
TILE = 256


def act(pre):
    return jax.nn.gelu(pre)


def dw_in_kernel(x_ref, d_pre_ref, dw_down_in, dw_in_ref, dw_down_ref, slab, load_sem, store_sem):
    step, steps = pl.program_id(0), pl.num_programs(0)
    height = slab.shape[1]
    slot = lax.rem(step, 2)

    def load(i, slot):
        rows = pl.ds(pl.multiple_of(i * height, height), height)
        return pltpu.make_async_copy(dw_down_in.at[rows], slab.at[slot], load_sem.at[slot])

    def store(i, slot):
        rows = pl.ds(pl.multiple_of(i * height, height), height)
        return pltpu.make_async_copy(slab.at[slot], dw_down_ref.at[rows], store_sem.at[slot])

    @pl.when(step >= 2)
    def _():
        store(step - 2, slot).wait()

    load(step, slot).start()
    dw_in_ref[...] = lax.dot_general(
        x_ref[...], d_pre_ref[...], (((0,), (0,)), ((), ())), preferred_element_type=jnp.float32
    ).astype(dw_in_ref.dtype)
    load(step, slot).wait()
    store(step, slot).start()

    @pl.when(step == steps - 1)
    def _():
        store(step - 1, 1 - slot).wait()
        store(step, slot).wait()


def dw_in_and_copy(x, d_pre, dw_down, tile):
    tokens, depth = x.shape
    width = d_pre.shape[1]
    steps = depth // tile
    height = dw_down.shape[0] // steps
    assert depth % tile == 0 and steps >= 2 and height * steps == dw_down.shape[0] and height % 16 == 0
    return pl.pallas_call(
        dw_in_kernel,
        grid=(steps,),
        in_specs=[
            pl.BlockSpec((tokens, tile), lambda i: (0, i)),
            pl.BlockSpec((tokens, width), lambda i: (0, 0)),
            pl.BlockSpec(memory_space=pl.ANY),
        ],
        out_specs=[pl.BlockSpec((tile, width), lambda i: (i, 0)), pl.BlockSpec(memory_space=pl.ANY)],
        out_shape=[jax.ShapeDtypeStruct((depth, width), x.dtype), jax.ShapeDtypeStruct(dw_down.shape, x.dtype)],
        scratch_shapes=[
            pltpu.VMEM((2, height, dw_down.shape[1]), x.dtype),
            pltpu.SemaphoreType.DMA((2,)),
            pltpu.SemaphoreType.DMA((2,)),
        ],
        compiler_params=pltpu.CompilerParams(vmem_limit_bytes=60 * 1024 * 1024),
        cost_estimate=pl.CostEstimate(
            flops=2 * tokens * depth * width,
            bytes_accessed=2 * (tokens * depth + tokens * width + 3 * depth * width),
            transcendentals=0,
        ),
    )(x, d_pre, dw_down)


STEPS = ((1, 0), (-1, 0), (0, 1), (0, -1))


class Torus:
    def __init__(self, side):
        self.side = side
        t, self.odd = lax.axis_index("tp"), lax.rem(lax.axis_index("dp"), 2)
        x, y = lax.div(t, side), lax.rem(t, side)
        self.me = tuple(m + self.odd * (self.mirror(n) - m) for m, n in ((x, y), (y, x)))

    def mirror(self, n):
        return lax.rem(self.side - n, self.side)

    def index(self, x, y):
        straight, mirrored = x * self.side + y, self.mirror(y) * self.side + self.mirror(x)
        return straight + self.odd * (mirrored - straight)

    def at(self, ox, oy):
        return self.index(*(lax.rem(m + o + self.side, self.side) for m, o in zip(self.me, (ox, oy))))


def pieces_of(link):
    along_x, up = link < 2, link % 2 == 0
    mine = (0, 1) if along_x else (2, 3)
    other = (2, 3) if along_x else (0, 1)
    if not up:
        mine, other = mine[::-1], other[::-1]
    back = -1 if up else 1

    def at(first, second):
        return (first, second) if along_x else (second, first)

    return (
        [(*at(0, 0), q) for q in mine + other],
        [(*at(back, 0), mine[0])],
        [(*at(0, s), q) for s, order in ((-1, (0, 1)), (1, (1, 0))) for q in (min(other) + order[0], min(other) + order[1])],
        [(*at(0, 2), q) for q in other],
        [(*at(back, s), other[0]) for s in (0, -1, 1, 2)],
    )


class Gather:
    def __init__(self, own, every, send_sem, recv_sem, torus):
        self.own, self.every, self.send_sem, self.recv_sem = own, every, send_sem, recv_sem
        self.torus, self.rows = torus, own.shape[0]
        self.unit = self.rows // 4
        self.sent, self.pending = [], {}
        for link, (dx, dy) in enumerate(STEPS):
            flat = [p for stage in pieces_of(link) for p in stage]
            for k, (ox, oy, q) in enumerate(flat):
                key = self.key(ox - dx, oy - dy, q)
                assert key not in self.pending
                self.pending[key] = (link, k)
        self.arrival = dict(self.pending)

    def key(self, ox, oy, q):
        return ox % self.torus.side, oy % self.torus.side, q

    def place(self, ox, oy, q):
        start = self.torus.at(*self.key(ox, oy, q)[:2]) * self.rows + q * self.unit
        return self.every.at[pl.ds(pl.multiple_of(start, 8), self.unit)]

    def copy(self, link, k, source, target):
        return pltpu.make_async_remote_copy(
            src_ref=source,
            dst_ref=target,
            send_sem=self.send_sem.at[link, k],
            recv_sem=self.recv_sem.at[link, k],
            device_id={"tp": self.torus.at(*STEPS[link])},
            device_id_type=MESH,
        )

    def arriving(self, ox, oy, q):
        found = self.pending.pop(self.key(ox, oy, q), None)
        place = self.place(ox, oy, q)
        return [] if found is None else [self.copy(*found, place, place)]

    def wait(self, ox, oy, q):
        for c in self.arriving(ox, oy, q):
            c.wait_recv()

    def send(self, stage, only=slice(None)):
        for before, copy in self.forwards(stage, only):
            for c in before:
                c.wait_recv()
            copy.start()

    def forwards(self, stage, only=slice(None)):
        copies = []
        todo = [(link, pieces_of(link)) for link in range(4)]
        count = len(todo[0][1][stage])
        for i in range(count)[only]:
            for link, stages in todo:
                k = sum(len(s) for s in stages[:stage]) + i
                ox, oy, q = stages[stage][i]
                place = self.place(ox, oy, q)
                if (ox, oy) == (0, 0):
                    before, source = [], self.own.at[pl.ds(q * self.unit, self.unit)]
                else:
                    before, source = self.arriving(ox, oy, q), place
                copies.append((before, self.copy(link, k, source, place)))
                self.sent.append((link, k, place))
        return copies

    def wait_shard(self, ox, oy):
        for q in range(4):
            self.wait(ox, oy, q)

    def finish_sends(self):
        for link, k, place in self.sent:
            self.copy(link, k, place, place).wait_send()
        self.sent.clear()

    def finish(self):
        for key in list(self.pending):
            self.wait(*key)
        self.finish_sends()


UP_DOWN = {"y": (2, 3), "x": (0, 1)}


def blocks_of(axis):
    up, down = UP_DOWN[axis]
    high, low = (0, 1) if axis == "y" else (2, 3)
    return {
        high: [(2, "relay", up), (1, "later", up), (-1, "direct", down), (0, "own", high)],
        low: [(2, "relay", down), (-1, "later", down), (1, "direct", up), (0, "own", low)],
    }


def barrier_with_neighbours(torus):
    barrier = pltpu.get_barrier_semaphore()
    for offset in STEPS:
        pl.semaphore_signal(barrier, inc=1, device_id={"tp": torus.at(*offset)}, device_id_type=MESH)
    pl.semaphore_wait(barrier, len(STEPS))


def run(copies):
    for c in copies:
        c.start()
    for c in copies:
        c.wait()


def gather_kernel(side, x_ref, dy_ref, pre_ref, w_down_ref, w_in_ref, x_all, dy_all, hidden_ref, d_pre_ref, dw_down_ref, *rest):
    relay, direct, direct_last, later, own_terms = (rest[4 * i : 4 * i + 4] for i in range(5))
    (
        weights, stage, dy_buf, pre_buf, hidden_buf, d_pre, narrow, wide, dy_tile,
        x_send, x_recv, dy_send, dy_recv, load_sem, store_sem, stage_sem, block_sem, tile_sem, out_sem,
    ) = rest[20:]
    rows, depth = dy_ref.shape
    width = pre_ref.shape[1]
    quarter = depth // 4
    torus = Torus(side)
    barrier_with_neighbours(torus)

    dys = Gather(dy_ref, dy_all, dy_send, dy_recv, torus)
    xs = Gather(x_ref, x_all, x_send, x_recv, torus)
    dys.send(0)

    def load_quarter(q):
        return pltpu.make_async_copy(w_in_ref.at[pl.ds(q * quarter, quarter)], stage, stage_sem)

    def tile_at(n, size=TILE):
        return pl.ds(n * size if isinstance(n, int) else pl.multiple_of(n * size, size), size)

    load_quarter(0).start()

    @pl.loop(0, width // TILE)
    def _(n):
        run([pltpu.make_async_copy(w_down_ref.at[tile_at(n)], dy_buf.at[pl.ds(0, TILE)], load_sem.at[0])])
        for k in range(4):
            weights[k, :, tile_at(n)] = dy_buf[0:TILE, k * quarter : (k + 1) * quarter].T

    def rows_of(ox, oy):
        return pl.ds(pl.multiple_of(torus.at(ox, oy) * rows, rows), rows)

    def wrap(offset):
        return offset % side if isinstance(offset, int) else lax.rem(offset + side, side)

    half = [pl.ds(0, rows), pl.ds(rows, rows)]
    stores = []

    def step_hidden(*pair, own=None):
        here = [rows_of(*offset) for offset in pair]
        at = [d_pre.at[wrap(ox), wrap(oy)] for ox, oy in pair]
        count = range(len(pair))
        run(
            [
                pltpu.make_async_copy(dy_ref if i == own else dy_all.at[here[i]], dy_buf.at[half[i]], load_sem.at[i])
                for i in count
            ]
            + [pltpu.make_async_copy(pre_ref.at[here[i]], pre_buf.at[half[i]], load_sem.at[2 + i]) for i in count]
        )
        flush()
        used = slice(0, len(pair) * rows)

        @pl.loop(0, width // TILE)
        def _(n):
            tile = tile_at(n)
            d_hidden = jnp.dot(
                dy_buf[used, :], weights[:, :, tile].reshape(depth, TILE), preferred_element_type=jnp.float32
            )
            hidden, back = jax.vjp(act, pre_buf[used, tile].astype(jnp.float32))
            hidden_buf[used, tile] = hidden.astype(hidden_buf.dtype)
            grad = back(d_hidden)[0].astype(d_pre.dtype)
            for i in count:
                at[i][:, tile] = grad[i * rows : (i + 1) * rows]

        for i in count:
            stores.append(pltpu.make_async_copy(hidden_buf.at[half[i]], hidden_ref.at[here[i]], store_sem.at[i]))
            stores.append(pltpu.make_async_copy(at[i], d_pre_ref.at[here[i]], store_sem.at[2 + i]))
            if i == own:
                stores.append(pltpu.make_async_copy(dy_buf.at[half[i]], dy_all.at[here[i]], store_sem.at[4]))
        for c in stores:
            c.start()

    def flush():
        for c in stores:
            c.wait()
        stores.clear()

    def steps_hidden(pair):
        flush()

        @pl.loop(0, 2)
        def _(k):
            step_hidden(*pair(k))
            flush()

    leaving = {0: [], 1: []}

    def step_dx(axis, q, offset, kind, index):
        exact = kind in ("later", "own")
        buf, which = (wide, 0) if exact else (narrow, 1)
        for c in leaving[which]:
            c.wait()

        @pl.loop(0, quarter // TILE)
        def _(n):
            tile = tile_at(n)
            lines = d_pre[:, offset % side] if axis == "y" else d_pre[offset % side]
            term = jnp.dot(lines.reshape(side * rows, width), weights[q, :, tile], preferred_element_type=jnp.float32)
            buf[:, :, tile] = term.astype(buf.dtype).reshape(side, rows, TILE)

        if kind == "direct":
            cut = [(buf.at[pl.ds(1, side - 1)], direct[index]), (buf.at[0], direct_last[index])]
        else:
            cut = [(buf, {"relay": relay, "later": later, "own": own_terms}[kind][index])]
        leaving[which] = [pltpu.make_async_copy(*c, block_sem.at[which, i]) for i, c in enumerate(cut)]
        for c in leaving[which]:
            c.start()

    dys.send(1)
    dys.send(2)
    step_hidden((0, 0), own=0)
    for offset in STEPS:
        dys.wait_shard(*offset)
    steps_hidden(lambda k: ((1 - k, k), (k - 1, -k)))
    dys.send(3)
    dys.send(4, slice(0, 3))
    for s in (1, -1):
        for offset in ((1, s), (-1, s)):
            dys.wait_shard(*offset)
        step_hidden((1, s), (-1, s))
        if s == 1:
            dys.send(4, slice(3, 4))
            xs.send(0)
    for shards in (((2, 0), (0, 2)), ((2, -1), (-1, 2)), ((2, 1), (1, 2)), ((2, 2),)):
        for offset in shards:
            dys.wait_shard(*offset)
        step_hidden(*shards)
    flush()
    own = dy_buf.at[half[0]]
    run([pltpu.make_async_copy(x_ref, own, load_sem.at[0])])
    stores.append(pltpu.make_async_copy(own, x_all.at[rows_of(0, 0)], store_sem.at[0]))
    stores[-1].start()
    tiles = dy_tile.shape[-1]

    def load_tile(n, slot):
        return pltpu.make_async_copy(dy_all.at[:, tile_at(n, tiles)], dy_tile.at[slot], tile_sem.at[slot])

    def store_tile(n, slot):
        return pltpu.make_async_copy(stage.at[:, tile_at(slot, tiles)], dw_down_ref.at[:, tile_at(n, tiles)], out_sem.at[slot])

    spare = side * side * rows - quarter
    hidden_loads = [
        pltpu.make_async_copy(hidden_ref.at[pl.ds(0, quarter)], weights.at[0], load_sem.at[1]),
        pltpu.make_async_copy(hidden_ref.at[pl.ds(quarter, spare)], weights.at[1, pl.ds(0, spare)], load_sem.at[2]),
    ]
    for axis in ("y", "x"):
        for q, blocks in blocks_of(axis).items():
            load_quarter(q).wait()

            @pl.loop(0, quarter // TILE)
            def _(n):
                weights[q, :, tile_at(n)] = stage[tile_at(n), :].T

            if q < 3:
                load_quarter(q + 1).start()
            else:
                for c in hidden_loads + [load_tile(0, 0)]:
                    c.start()
            for offset, kind, index in blocks:
                step_dx(axis, q, offset, kind, index)
            if q == 0:
                xs.send(1)
                xs.send(2)
            if q == 2:
                xs.send(3)
    for c in hidden_loads:
        c.wait()
    count = depth // tiles
    forwards = {4: xs.forwards(4, slice(0, 3)), 7: xs.forwards(4, slice(3, 4))}

    @pl.loop(0, count)
    def _(n):
        slot = lax.rem(n, 2)

        for when, copies in forwards.items():

            @pl.when(n == when)
            def _():
                for before, copy in copies:
                    for c in before:
                        c.wait_recv()
                    copy.start()

        @pl.when(n + 1 < count)
        def _():
            load_tile(n + 1, 1 - slot).start()

        @pl.when(n >= 2)
        def _():
            store_tile(n - 2, slot).wait()

        load_tile(n, slot).wait()
        hidden = jnp.concatenate([weights[0], weights[1, 0:spare, :]], axis=0)
        stage[:, tile_at(slot, tiles)] = lax.dot_general(
            hidden, dy_tile[slot], (((0,), (0,)), ((), ())), preferred_element_type=jnp.float32
        ).astype(stage.dtype)
        store_tile(n, slot).start()

    for c in stores + leaving[0] + leaving[1]:
        c.wait()
    for n in (count - 2, count - 1):
        store_tile(n, n % 2).wait()
    dys.finish()
    xs.finish_sends()
    xs.finish()


def gather_and_differentiate(x, dy, pre, w_down, w_in, group):
    side = math.isqrt(group)
    assert side == 4 and side * side == group
    rows, depth = dy.shape
    width = pre.shape[1]
    quarter, tile = depth // 4, 2 * TILE
    assert rows % 32 == 0 and width % TILE == 0 and quarter % TILE == 0 and depth // tile > 7
    assert quarter < group * rows <= 2 * quarter and width == quarter
    like = jax.ShapeDtypeStruct
    any_space = pl.BlockSpec(memory_space=pl.ANY)
    block = (side, rows, quarter)
    dma = pltpu.SemaphoreType.DMA
    outs = pl.pallas_call(
        functools.partial(gather_kernel, side),
        out_shape=[like((group * rows, depth), x.dtype)] * 2
        + [like((group * rows, width), x.dtype)] * 2
        + [like((width, depth), x.dtype)]
        + [like(block, x.dtype)] * 4
        + [like((side - 1, *block[1:]), x.dtype)] * 4
        + [like(block[1:], x.dtype)] * 4
        + [like(block, jnp.float32)] * 8,
        in_specs=[any_space] * 5,
        out_specs=[any_space] * 25,
        scratch_shapes=[
            pltpu.VMEM((4, quarter, width), x.dtype),
            pltpu.VMEM((quarter, width), x.dtype),
            pltpu.VMEM((2 * rows, depth), x.dtype),
            pltpu.VMEM((2 * rows, width), x.dtype),
            pltpu.VMEM((2 * rows, width), x.dtype),
            pltpu.VMEM((side, side, rows, width), x.dtype),
            pltpu.VMEM(block, x.dtype),
            pltpu.VMEM(block, jnp.float32),
            pltpu.VMEM((2, group * rows, tile), x.dtype),
            *[dma((4, 15))] * 4,
            dma((4,)),
            dma((5,)),
            dma,
            dma((2, 2)),
            dma((2,)),
            dma((2,)),
        ],
        compiler_params=pltpu.CompilerParams(
            collective_id=0, has_side_effects=True, vmem_limit_bytes=67_043_328
        ),
        cost_estimate=pl.CostEstimate(
            flops=6 * group * rows * depth * width,
            bytes_accessed=2 * (group * rows * (7 * depth + 4 * width) + 3 * depth * width),
            transcendentals=0,
        ),
        name="gather_and_differentiate",
    )(x, dy, pre, w_down, w_in)
    return *outs[:5], *(outs[5 + 4 * i : 9 + 4 * i] for i in range(5))


def shift(value, link, mesh):
    group = mesh.shape["tp"]
    side = math.isqrt(group)
    dx, dy = STEPS[link]
    pairs = []
    for g in range(mesh.shape["dp"]):
        index = (lambda x, y: -y % side * side + -x % side) if g % 2 else (lambda x, y: x * side + y)
        pairs += [
            (g * group + index(x, y), g * group + index((x + dx) % side, (y + dy) % side))
            for x in range(side)
            for y in range(side)
        ]
    return lax.ppermute(value, ("dp", "tp"), pairs)


def links_of_quarters():
    takes = {}
    for axis, other in (("y", "x"), ("x", "y")):
        (up, down), (cross_up, cross_down) = UP_DOWN[axis], UP_DOWN[other]
        high, low = (0, 1) if axis == "y" else (2, 3)
        takes[high] = up, down, cross_up, cross_down
        takes[low] = down, up, cross_down, cross_up
    return takes


def scatter_kernel(side, *refs):
    relay, direct, later, own_terms = (refs[4 * i : 4 * i + 4] for i in range(4))
    (
        kept_ref, last_ref, later_got, cross_got, later_out, cross_out, exact_in, narrow_in, sums,
        later_send, later_recv, cross_send, cross_recv, exact_sem, narrow_sem, kept_sem,
    ) = refs[16:]
    rows, quarter = exact_in.shape[1:]
    torus = Torus(side)
    barrier_with_neighbours(torus)

    def remote(link, source, target, send_sem, recv_sem):
        return pltpu.make_async_remote_copy(
            src_ref=source,
            dst_ref=target,
            send_sem=send_sem,
            recv_sem=recv_sem,
            device_id={"tp": torus.at(*STEPS[link])},
            device_id_type=MESH,
        )

    later_copies = {
        (link, j): remote(link, later_out.at[link, j], later_got.at[link, j], later_send.at[link, j], later_recv.at[link, j])
        for link in range(4)
        for j in range(side)
    }
    takes = links_of_quarters()
    step = lambda link: 1 if link in (0, 2) else side - 1
    columns = [pl.ds(q * quarter, quarter) for q in range(4)]
    cross_copies = {
        (q, k): remote(
            takes[q][3 if k == 1 else 2],
            cross_out.at[q, k],
            last_ref.at[:, columns[q]] if k == 2 else cross_got.at[q, k],
            cross_send.at[q, k],
            cross_recv.at[q, k],
        )
        for q in range(4)
        for k in range(3)
    }

    def add(target, *parts):
        strip = 16

        @pl.loop(0, rows // strip)
        def _(i):
            at = pl.ds(pl.multiple_of(i * strip, strip), strip)
            total = parts[0][at, :].astype(jnp.float32)
            for part in parts[1:]:
                total = total + part[at, :].astype(jnp.float32)
            target[at, :] = total.astype(target.dtype)

    order = [2, 1, side - 1, 0]
    tasks = [("later", link, j, later[link].at[j], relay[link].at[j]) for j in order for link in range(4)]
    for j in order:
        for q in range(4):
            link = takes[q][1]
            tasks.append(("sum", q, j, own_terms[q].at[j], None if j == 0 else direct[link].at[j - 1]))
    slots = exact_in.shape[0]

    def loads(n):
        _, _, _, exact, narrow = tasks[n]
        slot = n % slots
        copies = [pltpu.make_async_copy(exact, exact_in.at[slot], exact_sem.at[slot])]
        if narrow is not None:
            copies.append(pltpu.make_async_copy(narrow, narrow_in.at[slot], narrow_sem.at[slot]))
        return copies

    for n in range(slots - 1):
        for c in loads(n):
            c.start()
    for n, (kind, which, j, _, narrow) in enumerate(tasks):
        if n + slots - 1 < len(tasks):
            for c in loads(n + slots - 1):
                c.start()
        for c in loads(n):
            c.wait()
        exact, slot = exact_in.at[n % slots], n % slots
        if kind == "later":
            add(later_out.at[which, j], exact, narrow_in.at[slot])
            later_copies[which, j].start()
            continue
        q = which
        main, _, _, near_link = takes[q]
        later_copies[main, j].wait_recv()
        parts = [exact, later_got.at[main, j]]
        if narrow is not None:
            parts.append(narrow_in.at[slot])
        if j == 2:
            add(cross_out.at[q, 0], *parts)
            cross_copies[q, 0].start()
        elif j == step(near_link):
            add(cross_out.at[q, 1], *parts)
            cross_copies[q, 1].start()
        else:
            add(sums.at[q, 0 if j == 0 else 1], *parts)
    for q in range(4):
        cross_copies[q, 0].wait_recv()
        add(cross_out.at[q, 2], sums.at[q, 1], cross_got.at[q, 0])
        cross_copies[q, 2].start()
    outs = []
    for q in range(4):
        cross_copies[q, 1].wait_recv()
        add(sums.at[q, 1], sums.at[q, 0], cross_got.at[q, 1])
        outs.append(pltpu.make_async_copy(sums.at[q, 1], kept_ref.at[:, columns[q]], kept_sem.at[q]))
        outs[-1].start()
    for c in outs:
        c.wait()
    for c in [*later_copies.values(), *cross_copies.values()]:
        c.wait_send()
    for q in range(4):
        cross_copies[q, 2].wait_recv()


def sum_and_scatter(relay, direct, later, own_terms):
    side, rows, quarter = relay[0].shape
    kind = relay[0].dtype
    any_space = pl.BlockSpec(memory_space=pl.ANY)
    dma = pltpu.SemaphoreType.DMA
    piece, slots = (rows, quarter), 4
    return pl.pallas_call(
        functools.partial(scatter_kernel, side),
        out_shape=[jax.ShapeDtypeStruct((rows, 4 * quarter), t) for t in (jnp.float32, kind)],
        in_specs=[any_space] * 16,
        out_specs=[any_space] * 2,
        scratch_shapes=[
            pltpu.VMEM((4, side, *piece), kind),
            pltpu.VMEM((4, 2, *piece), kind),
            pltpu.VMEM((4, side, *piece), kind),
            pltpu.VMEM((4, 3, *piece), kind),
            pltpu.VMEM((slots, *piece), jnp.float32),
            pltpu.VMEM((slots, *piece), kind),
            pltpu.VMEM((4, 2, *piece), jnp.float32),
            dma((4, side)),
            dma((4, side)),
            dma((4, 3)),
            dma((4, 3)),
            dma((slots,)),
            dma((slots,)),
            dma((4,)),
        ],
        compiler_params=pltpu.CompilerParams(
            collective_id=1, has_side_effects=True, vmem_limit_bytes=67_043_328
        ),
        cost_estimate=pl.CostEstimate(
            flops=8 * side * rows * quarter, bytes_accessed=60 * side * rows * quarter, transcendentals=0
        ),
        name="sum_and_scatter",
    )(*relay, *direct, *later, *own_terms)


def finish_kernel(kept_ref, last_ref, *refs):
    direct, (dx_ref, kept, last, owner, dx, kept_sem, last_sem, owner_sem, dx_sem) = refs[:4], refs[4:]
    quarter = kept.shape[2]
    columns = [pl.ds(q * quarter, quarter) for q in range(4)]
    loads = [
        [
            pltpu.make_async_copy(kept_ref.at[:, columns[q]], kept.at[q], kept_sem.at[q]),
            pltpu.make_async_copy(last_ref.at[:, columns[q]], last.at[q], last_sem.at[q]),
            pltpu.make_async_copy(direct[q], owner.at[q], owner_sem.at[q]),
        ]
        for q in range(4)
    ]
    for copies in loads:
        for c in copies:
            c.start()
    stores = []
    for q, copies in enumerate(loads):
        for c in copies:
            c.wait()
        total = kept[q] + owner[q].astype(jnp.float32) + last[q].astype(jnp.float32)
        dx[q] = total.astype(dx.dtype)
        stores.append(pltpu.make_async_copy(dx.at[q], dx_ref.at[:, columns[q]], dx_sem.at[q]))
        stores[-1].start()
    for c in stores:
        c.wait()


def finish_dx(kept, last, direct_last):
    rows, depth = kept.shape
    pieces = (4, rows, depth // 4)
    takes = links_of_quarters()
    any_space = pl.BlockSpec(memory_space=pl.ANY)
    return pl.pallas_call(
        finish_kernel,
        in_specs=[any_space] * 6,
        out_specs=any_space,
        out_shape=jax.ShapeDtypeStruct(kept.shape, last.dtype),
        scratch_shapes=[pltpu.VMEM(pieces, jnp.float32)]
        + [pltpu.VMEM(pieces, last.dtype)] * 3
        + [pltpu.SemaphoreType.DMA((4,))] * 4,
        compiler_params=pltpu.CompilerParams(vmem_limit_bytes=60 * 1024 * 1024),
        cost_estimate=pl.CostEstimate(flops=2 * rows * depth, bytes_accessed=10 * rows * depth, transcendentals=0),
        name="finish_dx",
    )(kept, last, *(direct_last[takes[q][1]] for q in range(4)))


def solution(mesh):
    group = mesh.shape["tp"]

    def step(x, dy, pre, w_in, w_down):
        x_all, _, _, d_pre, dw_down, relay, direct, direct_last, later, own_terms = gather_and_differentiate(
            x, dy, pre, w_down, w_in, group
        )
        relay = [shift(block, link, mesh) for link, block in enumerate(relay)]
        direct = [shift(block, link, mesh) for link, block in enumerate(direct)]
        direct_last = [shift(block, link, mesh) for link, block in enumerate(direct_last)]
        dw_in, dw_down = dw_in_and_copy(x_all, d_pre, dw_down, 2 * TILE)
        dw_in, dw_down, later = lax.optimization_barrier((dw_in, dw_down, later))
        dx = finish_dx(*sum_and_scatter(relay, direct, later, own_terms), direct_last)
        return dx, dw_in, dw_down

    tokens = P(("dp", "tp"), None)
    step = jax.shard_map(
        step,
        mesh=mesh,
        in_specs=(tokens, tokens, P("dp", "tp"), P(None, "tp"), P("tp", None)),
        out_specs=(tokens, P("dp", "tp"), tokens),
        check_vma=False,
    )
    return step
```

```python
import functools
import math

import jax
import jax.numpy as jnp
from jax import lax
from jax.experimental import pallas as pl
from jax.experimental.pallas import tpu as pltpu
from jax.sharding import PartitionSpec as P


MESH = pl.DeviceIdType.MESH
TILE = 256


def act(pre):
    return jax.nn.gelu(pre)


def dw_in_kernel(x_ref, d_pre_ref, dw_down_in, dw_in_ref, dw_down_ref, slab, load_sem, store_sem):
    step, steps = pl.program_id(0), pl.num_programs(0)
    height = slab.shape[1]
    slot = lax.rem(step, 2)

    def load(i, slot):
        rows = pl.ds(pl.multiple_of(i * height, height), height)
        return pltpu.make_async_copy(dw_down_in.at[rows], slab.at[slot], load_sem.at[slot])

    def store(i, slot):
        rows = pl.ds(pl.multiple_of(i * height, height), height)
        return pltpu.make_async_copy(slab.at[slot], dw_down_ref.at[rows], store_sem.at[slot])

    @pl.when(step >= 2)
    def _():
        store(step - 2, slot).wait()

    load(step, slot).start()
    dw_in_ref[...] = lax.dot_general(
        x_ref[...], d_pre_ref[...], (((0,), (0,)), ((), ())), preferred_element_type=jnp.float32
    ).astype(dw_in_ref.dtype)
    load(step, slot).wait()
    store(step, slot).start()

    @pl.when(step == steps - 1)
    def _():
        store(step - 1, 1 - slot).wait()
        store(step, slot).wait()


def dw_in_and_copy(x, d_pre, dw_down, tile):
    tokens, depth = x.shape
    width = d_pre.shape[1]
    steps = depth // tile
    height = dw_down.shape[0] // steps
    assert depth % tile == 0 and steps >= 2 and height * steps == dw_down.shape[0] and height % 16 == 0
    return pl.pallas_call(
        dw_in_kernel,
        grid=(steps,),
        in_specs=[
            pl.BlockSpec((tokens, tile), lambda i: (0, i)),
            pl.BlockSpec((tokens, width), lambda i: (0, 0)),
            pl.BlockSpec(memory_space=pl.ANY),
        ],
        out_specs=[pl.BlockSpec((tile, width), lambda i: (i, 0)), pl.BlockSpec(memory_space=pl.ANY)],
        out_shape=[jax.ShapeDtypeStruct((depth, width), x.dtype), jax.ShapeDtypeStruct(dw_down.shape, x.dtype)],
        scratch_shapes=[
            pltpu.VMEM((2, height, dw_down.shape[1]), x.dtype),
            pltpu.SemaphoreType.DMA((2,)),
            pltpu.SemaphoreType.DMA((2,)),
        ],
        compiler_params=pltpu.CompilerParams(vmem_limit_bytes=60 * 1024 * 1024),
        cost_estimate=pl.CostEstimate(
            flops=2 * tokens * depth * width,
            bytes_accessed=2 * (tokens * depth + tokens * width + 3 * depth * width),
            transcendentals=0,
        ),
    )(x, d_pre, dw_down)


STEPS = ((1, 0), (-1, 0), (0, 1), (0, -1))


class Torus:
    def __init__(self, side):
        self.side = side
        t, self.odd = lax.axis_index("tp"), lax.rem(lax.axis_index("dp"), 2)
        x, y = lax.div(t, side), lax.rem(t, side)
        self.me = tuple(m + self.odd * (self.mirror(n) - m) for m, n in ((x, y), (y, x)))

    def mirror(self, n):
        return lax.rem(self.side - n, self.side)

    def index(self, x, y):
        straight, mirrored = x * self.side + y, self.mirror(y) * self.side + self.mirror(x)
        return straight + self.odd * (mirrored - straight)

    def at(self, ox, oy):
        return self.index(*(lax.rem(m + o + self.side, self.side) for m, o in zip(self.me, (ox, oy))))


def pieces_of(link):
    along_x, up = link < 2, link % 2 == 0
    mine = (0, 1) if along_x else (2, 3)
    other = (2, 3) if along_x else (0, 1)
    if not up:
        mine, other = mine[::-1], other[::-1]
    back = -1 if up else 1

    def at(first, second):
        return (first, second) if along_x else (second, first)

    return (
        [(*at(0, 0), q) for q in mine + other],
        [(*at(back, 0), mine[0])],
        [(*at(0, s), q) for s, order in ((-1, (0, 1)), (1, (1, 0))) for q in (min(other) + order[0], min(other) + order[1])],
        [(*at(0, 2), q) for q in other],
        [(*at(back, s), other[0]) for s in (0, -1, 1, 2)],
    )


class Gather:
    def __init__(self, own, every, send_sem, recv_sem, torus):
        self.own, self.every, self.send_sem, self.recv_sem = own, every, send_sem, recv_sem
        self.torus, self.rows = torus, own.shape[0]
        self.unit = self.rows // 4
        self.sent, self.pending = [0] * 4, {}
        for link, (dx, dy) in enumerate(STEPS):
            flat = [p for stage in pieces_of(link) for p in stage]
            for k, (ox, oy, q) in enumerate(flat):
                key = self.key(ox - dx, oy - dy, q)
                assert key not in self.pending
                self.pending[key] = (link, k)
        self.arrival = dict(self.pending)

    def key(self, ox, oy, q):
        return ox % self.torus.side, oy % self.torus.side, q

    def place(self, ox, oy, q):
        start = self.torus.at(*self.key(ox, oy, q)[:2]) * self.rows + q * self.unit
        return self.every.at[pl.ds(pl.multiple_of(start, 8), self.unit)]

    def copy(self, link, k, source, target):
        return pltpu.make_async_remote_copy(
            src_ref=source,
            dst_ref=target,
            send_sem=self.send_sem.at[link],
            recv_sem=self.recv_sem.at[link, k],
            device_id={"tp": self.torus.at(*STEPS[link])},
            device_id_type=MESH,
        )

    def arriving(self, ox, oy, q):
        found = self.pending.pop(self.key(ox, oy, q), None)
        place = self.place(ox, oy, q)
        return [] if found is None else [self.copy(*found, place, place)]

    def wait(self, ox, oy, q):
        for c in self.arriving(ox, oy, q):
            c.wait_recv()

    def send(self, stage, only=slice(None)):
        for before, copy in self.forwards(stage, only):
            for c in before:
                c.wait_recv()
            copy.start()

    def forwards(self, stage, only=slice(None)):
        copies = []
        todo = [(link, pieces_of(link)) for link in range(4)]
        count = len(todo[0][1][stage])
        for i in range(count)[only]:
            for link, stages in todo:
                k = sum(len(s) for s in stages[:stage]) + i
                ox, oy, q = stages[stage][i]
                place = self.place(ox, oy, q)
                if (ox, oy) == (0, 0):
                    before, source = [], self.own.at[pl.ds(q * self.unit, self.unit)]
                else:
                    before, source = self.arriving(ox, oy, q), place
                copies.append((before, self.copy(link, k, source, place)))
                self.sent[link] += 1
        return copies

    def wait_shard(self, ox, oy):
        for q in range(4):
            self.wait(ox, oy, q)

    def finish_sends(self):
        for link, count in enumerate(self.sent):
            if count:
                sent = self.every.at[pl.ds(0, count * self.unit)]
                self.copy(link, 0, sent, sent).wait_send()
        self.sent = [0] * 4

    def finish(self):
        for key in list(self.pending):
            self.wait(*key)
        self.finish_sends()


UP_DOWN = {"y": (2, 3), "x": (0, 1)}


def blocks_of(axis):
    up, down = UP_DOWN[axis]
    high, low = (0, 1) if axis == "y" else (2, 3)
    return {
        high: [(2, "relay", up), (1, "later", up), (-1, "direct", down), (0, "own", high)],
        low: [(2, "relay", down), (-1, "later", down), (1, "direct", up), (0, "own", low)],
    }


def barrier_with_neighbours(torus):
    barrier = pltpu.get_barrier_semaphore()
    for offset in STEPS:
        pl.semaphore_signal(barrier, inc=1, device_id={"tp": torus.at(*offset)}, device_id_type=MESH)
    pl.semaphore_wait(barrier, len(STEPS))


def run(copies):
    for c in copies:
        c.start()
    for c in copies:
        c.wait()


def gather_kernel(side, x_ref, dy_ref, pre_ref, w_down_ref, w_in_ref, x_all, dy_all, hidden_ref, d_pre_ref, dw_down_ref, *rest):
    relay, direct, direct_last, later, own_terms = (rest[4 * i : 4 * i + 4] for i in range(5))
    (
        weights, stage, dy_buf, pre_buf, hidden_buf, d_pre, narrow, wide, dy_tile,
        x_send, x_recv, dy_send, dy_recv, load_sem, store_sem, stage_sem, block_sem, tile_sem, out_sem,
    ) = rest[20:]
    rows, depth = dy_ref.shape
    width = pre_ref.shape[1]
    quarter = depth // 4
    torus = Torus(side)
    barrier_with_neighbours(torus)

    dys = Gather(dy_ref, dy_all, dy_send, dy_recv, torus)
    xs = Gather(x_ref, x_all, x_send, x_recv, torus)
    dys.send(0)

    def load_quarter(q):
        return pltpu.make_async_copy(w_in_ref.at[pl.ds(q * quarter, quarter)], stage, stage_sem)

    def tile_at(n, size=TILE):
        return pl.ds(n * size if isinstance(n, int) else pl.multiple_of(n * size, size), size)

    load_quarter(0).start()

    @pl.loop(0, width // TILE)
    def _(n):
        run([pltpu.make_async_copy(w_down_ref.at[tile_at(n)], dy_buf.at[pl.ds(0, TILE)], load_sem.at[0])])
        for k in range(4):
            weights[k, :, tile_at(n)] = dy_buf[0:TILE, k * quarter : (k + 1) * quarter].T

    def rows_of(ox, oy):
        return pl.ds(pl.multiple_of(torus.at(ox, oy) * rows, rows), rows)

    def wrap(offset):
        return offset % side if isinstance(offset, int) else lax.rem(offset + side, side)

    half = [pl.ds(0, rows), pl.ds(rows, rows)]
    stores = []

    def step_hidden(*pair, own=None):
        here = [rows_of(*offset) for offset in pair]
        at = [d_pre.at[wrap(ox), wrap(oy)] for ox, oy in pair]
        count = range(len(pair))
        run(
            [
                pltpu.make_async_copy(dy_ref if i == own else dy_all.at[here[i]], dy_buf.at[half[i]], load_sem.at[i])
                for i in count
            ]
            + [pltpu.make_async_copy(pre_ref.at[here[i]], pre_buf.at[half[i]], load_sem.at[2 + i]) for i in count]
        )
        flush()
        used = slice(0, len(pair) * rows)

        @pl.loop(0, width // TILE)
        def _(n):
            tile = tile_at(n)
            d_hidden = jnp.dot(
                dy_buf[used, :], weights[:, :, tile].reshape(depth, TILE), preferred_element_type=jnp.float32
            )
            hidden, back = jax.vjp(act, pre_buf[used, tile].astype(jnp.float32))
            hidden_buf[used, tile] = hidden.astype(hidden_buf.dtype)
            grad = back(d_hidden)[0].astype(d_pre.dtype)
            for i in count:
                at[i][:, tile] = grad[i * rows : (i + 1) * rows]

        for i in count:
            stores.append(pltpu.make_async_copy(hidden_buf.at[half[i]], hidden_ref.at[here[i]], store_sem.at[i]))
            stores.append(pltpu.make_async_copy(at[i], d_pre_ref.at[here[i]], store_sem.at[2 + i]))
            if i == own:
                stores.append(pltpu.make_async_copy(dy_buf.at[half[i]], dy_all.at[here[i]], store_sem.at[4]))
        for c in stores:
            c.start()

    def flush():
        for c in stores:
            c.wait()
        stores.clear()

    def steps_hidden(pair):
        flush()

        @pl.loop(0, 2)
        def _(k):
            step_hidden(*pair(k))
            flush()

    leaving = {0: [], 1: []}

    def step_dx(axis, q, offset, kind, index):
        exact = kind in ("later", "own")
        buf, which = (wide, 0) if exact else (narrow, 1)
        for c in leaving[which]:
            c.wait()

        @pl.loop(0, quarter // TILE)
        def _(n):
            tile = tile_at(n)
            lines = d_pre[:, offset % side] if axis == "y" else d_pre[offset % side]
            term = jnp.dot(lines.reshape(side * rows, width), weights[q, :, tile], preferred_element_type=jnp.float32)
            buf[:, :, tile] = term.astype(buf.dtype).reshape(side, rows, TILE)

        if kind == "direct":
            cut = [(buf.at[pl.ds(1, side - 1)], direct[index]), (buf.at[0], direct_last[index])]
        else:
            cut = [(buf, {"relay": relay, "later": later, "own": own_terms}[kind][index])]
        leaving[which] = [pltpu.make_async_copy(*c, block_sem.at[which, i]) for i, c in enumerate(cut)]
        for c in leaving[which]:
            c.start()

    dys.send(1)
    dys.send(2)
    step_hidden((0, 0), own=0)
    for offset in STEPS:
        dys.wait_shard(*offset)
    steps_hidden(lambda k: ((1 - k, k), (k - 1, -k)))
    dys.send(3)
    dys.send(4, slice(0, 3))
    for s in (1, -1):
        for offset in ((1, s), (-1, s)):
            dys.wait_shard(*offset)
        step_hidden((1, s), (-1, s))
        if s == 1:
            dys.send(4, slice(3, 4))
            xs.send(0)
    for shards in (((2, 0), (0, 2)), ((2, -1), (-1, 2)), ((2, 1), (1, 2)), ((2, 2),)):
        for offset in shards:
            dys.wait_shard(*offset)
        step_hidden(*shards)
    flush()
    own = dy_buf.at[half[0]]
    run([pltpu.make_async_copy(x_ref, own, load_sem.at[0])])
    stores.append(pltpu.make_async_copy(own, x_all.at[rows_of(0, 0)], store_sem.at[0]))
    stores[-1].start()
    tiles = dy_tile.shape[-1]

    def load_tile(n, slot):
        return pltpu.make_async_copy(dy_all.at[:, tile_at(n, tiles)], dy_tile.at[slot], tile_sem.at[slot])

    def store_tile(n, slot):
        return pltpu.make_async_copy(stage.at[:, tile_at(slot, tiles)], dw_down_ref.at[:, tile_at(n, tiles)], out_sem.at[slot])

    spare = side * side * rows - quarter
    hidden_loads = [
        pltpu.make_async_copy(hidden_ref.at[pl.ds(0, quarter)], weights.at[0], load_sem.at[1]),
        pltpu.make_async_copy(hidden_ref.at[pl.ds(quarter, spare)], weights.at[1, pl.ds(0, spare)], load_sem.at[2]),
    ]
    for axis in ("y", "x"):
        for q, blocks in blocks_of(axis).items():
            load_quarter(q).wait()

            @pl.loop(0, quarter // TILE)
            def _(n):
                weights[q, :, tile_at(n)] = stage[tile_at(n), :].T

            if q < 3:
                load_quarter(q + 1).start()
            else:
                for c in hidden_loads + [load_tile(0, 0)]:
                    c.start()
            for offset, kind, index in blocks:
                step_dx(axis, q, offset, kind, index)
            if q == 0:
                xs.send(1)
                xs.send(2)
            if q == 2:
                xs.send(3)
    for c in hidden_loads:
        c.wait()
    count = depth // tiles
    forwards = {4: xs.forwards(4, slice(0, 3)), 7: xs.forwards(4, slice(3, 4))}

    @pl.loop(0, count)
    def _(n):
        slot = lax.rem(n, 2)

        for when, copies in forwards.items():

            @pl.when(n == when)
            def _():
                for before, copy in copies:
                    for c in before:
                        c.wait_recv()
                    copy.start()

        @pl.when(n + 1 < count)
        def _():
            load_tile(n + 1, 1 - slot).start()

        @pl.when(n >= 2)
        def _():
            store_tile(n - 2, slot).wait()

        load_tile(n, slot).wait()
        hidden = jnp.concatenate([weights[0], weights[1, 0:spare, :]], axis=0)
        stage[:, tile_at(slot, tiles)] = lax.dot_general(
            hidden, dy_tile[slot], (((0,), (0,)), ((), ())), preferred_element_type=jnp.float32
        ).astype(stage.dtype)
        store_tile(n, slot).start()

    for c in stores + leaving[0] + leaving[1]:
        c.wait()
    for n in (count - 2, count - 1):
        store_tile(n, n % 2).wait()
    dys.finish()
    xs.finish_sends()
    xs.finish()


def gather_and_differentiate(x, dy, pre, w_down, w_in, group):
    side = math.isqrt(group)
    assert side == 4 and side * side == group
    rows, depth = dy.shape
    width = pre.shape[1]
    quarter, tile = depth // 4, 2 * TILE
    assert rows % 32 == 0 and width % TILE == 0 and quarter % TILE == 0 and depth // tile > 7
    assert quarter < group * rows <= 2 * quarter and width == quarter
    like = jax.ShapeDtypeStruct
    any_space = pl.BlockSpec(memory_space=pl.ANY)
    block = (side, rows, quarter)
    dma = pltpu.SemaphoreType.DMA
    outs = pl.pallas_call(
        functools.partial(gather_kernel, side),
        out_shape=[like((group * rows, depth), x.dtype)] * 2
        + [like((group * rows, width), x.dtype)] * 2
        + [like((width, depth), x.dtype)]
        + [like(block, x.dtype)] * 4
        + [like((side - 1, *block[1:]), x.dtype)] * 4
        + [like(block[1:], x.dtype)] * 4
        + [like(block, jnp.float32)] * 8,
        in_specs=[any_space] * 5,
        out_specs=[any_space] * 25,
        scratch_shapes=[
            pltpu.VMEM((4, quarter, width), x.dtype),
            pltpu.VMEM((quarter, width), x.dtype),
            pltpu.VMEM((2 * rows, depth), x.dtype),
            pltpu.VMEM((2 * rows, width), x.dtype),
            pltpu.VMEM((2 * rows, width), x.dtype),
            pltpu.VMEM((side, side, rows, width), x.dtype),
            pltpu.VMEM(block, x.dtype),
            pltpu.VMEM(block, jnp.float32),
            pltpu.VMEM((2, group * rows, tile), x.dtype),
            *[dma((4,)), dma((4, 15))] * 2,
            dma((4,)),
            dma((5,)),
            dma,
            dma((2, 2)),
            dma((2,)),
            dma((2,)),
        ],
        compiler_params=pltpu.CompilerParams(
            collective_id=0, has_side_effects=True, vmem_limit_bytes=67_043_328
        ),
        cost_estimate=pl.CostEstimate(
            flops=6 * group * rows * depth * width,
            bytes_accessed=2 * (group * rows * (7 * depth + 4 * width) + 3 * depth * width),
            transcendentals=0,
        ),
        name="gather_and_differentiate",
    )(x, dy, pre, w_down, w_in)
    return *outs[:5], *(outs[5 + 4 * i : 9 + 4 * i] for i in range(5))


def shift(value, link, mesh):
    group = mesh.shape["tp"]
    side = math.isqrt(group)
    dx, dy = STEPS[link]
    pairs = []
    for g in range(mesh.shape["dp"]):
        index = (lambda x, y: -y % side * side + -x % side) if g % 2 else (lambda x, y: x * side + y)
        pairs += [
            (g * group + index(x, y), g * group + index((x + dx) % side, (y + dy) % side))
            for x in range(side)
            for y in range(side)
        ]
    return lax.ppermute(value, ("dp", "tp"), pairs)


def links_of_quarters():
    takes = {}
    for axis, other in (("y", "x"), ("x", "y")):
        (up, down), (cross_up, cross_down) = UP_DOWN[axis], UP_DOWN[other]
        high, low = (0, 1) if axis == "y" else (2, 3)
        takes[high] = up, down, cross_up, cross_down
        takes[low] = down, up, cross_down, cross_up
    return takes


def scatter_kernel(side, *refs):
    relay, direct, later, own_terms = (refs[4 * i : 4 * i + 4] for i in range(4))
    (
        kept_ref, last_ref, later_got, cross_got, later_out, cross_out, exact_in, narrow_in, sums,
        later_send, later_recv, cross_send, cross_recv, exact_sem, narrow_sem,
    ) = refs[16:]
    rows, quarter = exact_in.shape[1:]
    torus = Torus(side)
    barrier_with_neighbours(torus)

    def remote(link, source, target, send_sem, recv_sem):
        return pltpu.make_async_remote_copy(
            src_ref=source,
            dst_ref=target,
            send_sem=send_sem,
            recv_sem=recv_sem,
            device_id={"tp": torus.at(*STEPS[link])},
            device_id_type=MESH,
        )

    later_copies = {
        (link, j): remote(link, later_out.at[link, j], later_got.at[link, j], later_send.at[link], later_recv.at[link, j])
        for link in range(4)
        for j in range(side)
    }
    takes = links_of_quarters()
    step = lambda link: 1 if link in (0, 2) else side - 1
    columns = [pl.ds(q * quarter, quarter) for q in range(4)]
    cross_copies = {
        (q, k): remote(
            takes[q][3 if k == 1 else 2],
            cross_out.at[q, k],
            last_ref.at[:, columns[q]] if k == 2 else cross_got.at[q, k],
            cross_send.at[q],
            cross_recv.at[q, k],
        )
        for q in range(4)
        for k in range(3)
    }

    def add(target, *parts):
        strip = 16

        @pl.loop(0, rows // strip)
        def _(i):
            at = pl.ds(pl.multiple_of(i * strip, strip), strip)
            total = parts[0][at, :].astype(jnp.float32)
            for part in parts[1:]:
                total = total + part[at, :].astype(jnp.float32)
            target[at, :] = total.astype(target.dtype)

    order = [2, 1, side - 1, 0]
    tasks = [("later", link, j, later[link].at[j], relay[link].at[j]) for j in order for link in range(4)]
    for j in order:
        for q in range(4):
            link = takes[q][1]
            tasks.append(("sum", q, j, own_terms[q].at[j], None if j == 0 else direct[link].at[j - 1]))
    slots = exact_in.shape[0]

    def loads(n):
        _, _, _, exact, narrow = tasks[n]
        slot = n % slots
        copies = [pltpu.make_async_copy(exact, exact_in.at[slot], exact_sem.at[slot])]
        if narrow is not None:
            copies.append(pltpu.make_async_copy(narrow, narrow_in.at[slot], narrow_sem.at[slot]))
        return copies

    for n in range(slots - 1):
        for c in loads(n):
            c.start()
    for n, (kind, which, j, _, narrow) in enumerate(tasks):
        if n + slots - 1 < len(tasks):
            for c in loads(n + slots - 1):
                c.start()
        for c in loads(n):
            c.wait()
        exact, slot = exact_in.at[n % slots], n % slots
        if kind == "later":
            add(later_out.at[which, j], exact, narrow_in.at[slot])
            later_copies[which, j].start()
            continue
        q = which
        main, _, _, near_link = takes[q]
        later_copies[main, j].wait_recv()
        parts = [exact, later_got.at[main, j]]
        if narrow is not None:
            parts.append(narrow_in.at[slot])
        if j == 2:
            add(cross_out.at[q, 0], *parts)
            cross_copies[q, 0].start()
        elif j == step(near_link):
            add(cross_out.at[q, 1], *parts)
            cross_copies[q, 1].start()
        else:
            add(sums.at[q, 0 if j == 0 else 1], *parts)
    for q in range(4):
        cross_copies[q, 0].wait_recv()
        add(cross_out.at[q, 2], sums.at[q, 1], cross_got.at[q, 0])
        cross_copies[q, 2].start()
    for q in range(4):
        cross_copies[q, 1].wait_recv()
        add(kept_ref.at[:, columns[q]], sums.at[q, 0], cross_got.at[q, 1])
    for link in range(4):
        remote(link, later_out.at[link], later_out.at[link], later_send.at[link], later_recv.at[link, 0]).wait_send()
    for q in range(4):
        remote(takes[q][2], cross_out.at[q], cross_out.at[q], cross_send.at[q], cross_recv.at[q, 0]).wait_send()
    for q in range(4):
        cross_copies[q, 2].wait_recv()


def sum_and_scatter(relay, direct, later, own_terms):
    side, rows, quarter = relay[0].shape
    kind = relay[0].dtype
    any_space = pl.BlockSpec(memory_space=pl.ANY)
    dma = pltpu.SemaphoreType.DMA
    piece, slots = (rows, quarter), 4
    return pl.pallas_call(
        functools.partial(scatter_kernel, side),
        out_shape=[pltpu.VMEM((rows, 4 * quarter), t) for t in (jnp.float32, kind)],
        in_specs=[any_space] * 16,
        out_specs=[pl.BlockSpec(memory_space=pltpu.VMEM)] * 2,
        scratch_shapes=[
            pltpu.VMEM((4, side, *piece), kind),
            pltpu.VMEM((4, 2, *piece), kind),
            pltpu.VMEM((4, side, *piece), kind),
            pltpu.VMEM((4, 3, *piece), kind),
            pltpu.VMEM((slots, *piece), jnp.float32),
            pltpu.VMEM((slots, *piece), kind),
            pltpu.VMEM((4, 2, *piece), jnp.float32),
            dma((4,)),
            dma((4, side)),
            dma((4,)),
            dma((4, 3)),
            dma((slots,)),
            dma((slots,)),
        ],
        compiler_params=pltpu.CompilerParams(
            collective_id=1, has_side_effects=True, vmem_limit_bytes=54 * 1024 * 1024
        ),
        cost_estimate=pl.CostEstimate(
            flops=8 * side * rows * quarter, bytes_accessed=60 * side * rows * quarter, transcendentals=0
        ),
        name="sum_and_scatter",
    )(*relay, *direct, *later, *own_terms)


def finish_kernel(kept_ref, last_ref, *refs):
    direct, (dx_ref, owner, dx, owner_sem, dx_sem) = refs[:4], refs[4:]
    quarter = owner.shape[2]
    columns = [pl.ds(q * quarter, quarter) for q in range(4)]
    loads = [
        [
            pltpu.make_async_copy(direct[q], owner.at[q], owner_sem.at[q]),
        ]
        for q in range(4)
    ]
    for copies in loads:
        for c in copies:
            c.start()
    stores = []
    for q, copies in enumerate(loads):
        for c in copies:
            c.wait()
        total = kept_ref[:, columns[q]] + owner[q].astype(jnp.float32) + last_ref[:, columns[q]].astype(jnp.float32)
        dx[q] = total.astype(dx.dtype)
        stores.append(pltpu.make_async_copy(dx.at[q], dx_ref.at[:, columns[q]], dx_sem.at[q]))
        stores[-1].start()
    for c in stores:
        c.wait()


def finish_dx(kept, last, direct_last):
    rows, depth = kept.shape
    pieces = (4, rows, depth // 4)
    takes = links_of_quarters()
    any_space = pl.BlockSpec(memory_space=pl.ANY)
    return pl.pallas_call(
        finish_kernel,
        in_specs=[pl.BlockSpec(memory_space=pltpu.VMEM)] * 2 + [any_space] * 4,
        out_specs=any_space,
        out_shape=jax.ShapeDtypeStruct(kept.shape, last.dtype),
        scratch_shapes=[pltpu.VMEM(pieces, last.dtype)] * 2 + [pltpu.SemaphoreType.DMA((4,))] * 2,
        compiler_params=pltpu.CompilerParams(vmem_limit_bytes=32 * 1024 * 1024),
        cost_estimate=pl.CostEstimate(flops=2 * rows * depth, bytes_accessed=10 * rows * depth, transcendentals=0),
        name="finish_dx",
    )(kept, last, *(direct_last[takes[q][1]] for q in range(4)))


def solution(mesh):
    group = mesh.shape["tp"]

    def step(x, dy, pre, w_in, w_down):
        x_all, _, _, d_pre, dw_down, relay, direct, direct_last, later, own_terms = gather_and_differentiate(
            x, dy, pre, w_down, w_in, group
        )
        relay = [shift(block, link, mesh) for link, block in enumerate(relay)]
        direct = [shift(block, link, mesh) for link, block in enumerate(direct)]
        direct_last = [shift(block, link, mesh) for link, block in enumerate(direct_last)]
        dw_in, dw_down = dw_in_and_copy(x_all, d_pre, dw_down, 2 * TILE)
        dw_in, dw_down, later = lax.optimization_barrier((dw_in, dw_down, later))
        dx = finish_dx(*sum_and_scatter(relay, direct, later, own_terms), direct_last)
        return dx, dw_in, dw_down

    tokens = P(("dp", "tp"), None)
    step = jax.shard_map(
        step,
        mesh=mesh,
        in_specs=(tokens, tokens, P("dp", "tp"), P(None, "tp"), P("tp", None)),
        out_specs=(tokens, P("dp", "tp"), tokens),
        check_vma=False,
    )
    return step
```

```python
import functools
import math

import jax
import jax.numpy as jnp
from jax import lax
from jax.experimental import pallas as pl
from jax.experimental.pallas import tpu as pltpu
from jax.sharding import PartitionSpec as P


MESH = pl.DeviceIdType.MESH
TILE = 256


def act(pre):
    return jax.nn.gelu(pre)


def dw_in_kernel(x_ref, d_pre_ref, dw_down_in, dw_in_ref, dw_down_ref, slab, load_sem, store_sem):
    step, steps = pl.program_id(0), pl.num_programs(0)
    height = slab.shape[1]
    slot = lax.rem(step, 2)

    def load(i, slot):
        rows = pl.ds(pl.multiple_of(i * height, height), height)
        return pltpu.make_async_copy(dw_down_in.at[rows], slab.at[slot], load_sem.at[slot])

    def store(i, slot):
        rows = pl.ds(pl.multiple_of(i * height, height), height)
        return pltpu.make_async_copy(slab.at[slot], dw_down_ref.at[rows], store_sem.at[slot])

    @pl.when(step >= 2)
    def _():
        store(step - 2, slot).wait()

    load(step, slot).start()
    dw_in_ref[...] = lax.dot_general(
        x_ref[...], d_pre_ref[...], (((0,), (0,)), ((), ())), preferred_element_type=jnp.float32
    ).astype(dw_in_ref.dtype)
    load(step, slot).wait()
    store(step, slot).start()

    @pl.when(step == steps - 1)
    def _():
        store(step - 1, 1 - slot).wait()
        store(step, slot).wait()


def dw_in_and_copy(x, d_pre, dw_down, tile):
    tokens, depth = x.shape
    width = d_pre.shape[1]
    steps = depth // tile
    height = dw_down.shape[0] // steps
    assert depth % tile == 0 and steps >= 2 and height * steps == dw_down.shape[0] and height % 16 == 0
    return pl.pallas_call(
        dw_in_kernel,
        grid=(steps,),
        in_specs=[
            pl.BlockSpec((tokens, tile), lambda i: (0, i)),
            pl.BlockSpec((tokens, width), lambda i: (0, 0)),
            pl.BlockSpec(memory_space=pl.ANY),
        ],
        out_specs=[pl.BlockSpec((tile, width), lambda i: (i, 0)), pl.BlockSpec(memory_space=pl.ANY)],
        out_shape=[jax.ShapeDtypeStruct((depth, width), x.dtype), jax.ShapeDtypeStruct(dw_down.shape, x.dtype)],
        scratch_shapes=[
            pltpu.VMEM((2, height, dw_down.shape[1]), x.dtype),
            pltpu.SemaphoreType.DMA((2,)),
            pltpu.SemaphoreType.DMA((2,)),
        ],
        compiler_params=pltpu.CompilerParams(vmem_limit_bytes=60 * 1024 * 1024),
        cost_estimate=pl.CostEstimate(
            flops=2 * tokens * depth * width,
            bytes_accessed=2 * (tokens * depth + tokens * width + 3 * depth * width),
            transcendentals=0,
        ),
    )(x, d_pre, dw_down)


STEPS = ((1, 0), (-1, 0), (0, 1), (0, -1))


class Torus:
    def __init__(self, side):
        self.side = side
        t, self.odd = lax.axis_index("tp"), lax.rem(lax.axis_index("dp"), 2)
        x, y = lax.div(t, side), lax.rem(t, side)
        self.me = tuple(m + self.odd * (self.mirror(n) - m) for m, n in ((x, y), (y, x)))

    def mirror(self, n):
        return lax.rem(self.side - n, self.side)

    def index(self, x, y):
        straight, mirrored = x * self.side + y, self.mirror(y) * self.side + self.mirror(x)
        return straight + self.odd * (mirrored - straight)

    def at(self, ox, oy):
        return self.index(*(lax.rem(m + o + self.side, self.side) for m, o in zip(self.me, (ox, oy))))


def pieces_of(link):
    along_x, up = link < 2, link % 2 == 0
    mine = (0, 1) if along_x else (2, 3)
    other = (2, 3) if along_x else (0, 1)
    if not up:
        mine, other = mine[::-1], other[::-1]
    back = -1 if up else 1

    def at(first, second):
        return (first, second) if along_x else (second, first)

    return (
        [(*at(0, 0), q) for q in mine + other],
        [(*at(back, 0), mine[0])],
        [(*at(0, s), q) for s, order in ((-1, (0, 1)), (1, (1, 0))) for q in (min(other) + order[0], min(other) + order[1])],
        [(*at(0, 2), q) for q in other],
        [(*at(back, s), other[0]) for s in (0, -1, 1, 2)],
    )


TOGETHER = (0, 1), (2, 3), (4,), (5, 6, 7, 8), (9, 10), (11, 12, 13, 14)
APART = *TOGETHER[:-1], (11,), (12,), (13,), (14,)


class Gather:
    def __init__(self, own, every, send_sem, recv_sem, torus, groups):
        self.groups = groups
        self.group_of = {k: g for g, pieces in enumerate(groups) for k in pieces}
        self.own, self.every, self.send_sem, self.recv_sem = own, every, send_sem, recv_sem
        self.torus, self.rows = torus, own.shape[0]
        self.unit = self.rows // 4
        self.sent, self.pending = [0] * 4, {}
        for link, (dx, dy) in enumerate(STEPS):
            flat = [p for stage in pieces_of(link) for p in stage]
            for k, (ox, oy, q) in enumerate(flat):
                key = self.key(ox - dx, oy - dy, q)
                assert key not in self.pending
                self.pending[key] = (link, k)

    def key(self, ox, oy, q):
        return ox % self.torus.side, oy % self.torus.side, q

    def place(self, ox, oy, q):
        start = self.torus.at(*self.key(ox, oy, q)[:2]) * self.rows + q * self.unit
        return self.every.at[pl.ds(pl.multiple_of(start, 8), self.unit)]

    def copy(self, link, k, source, target):
        return pltpu.make_async_remote_copy(
            src_ref=source,
            dst_ref=target,
            send_sem=self.send_sem.at[link],
            recv_sem=self.recv_sem.at[link, self.group_of[k]],
            device_id={"tp": self.torus.at(*STEPS[link])},
            device_id_type=MESH,
        )

    def arriving(self, ox, oy, q):
        if self.key(ox, oy, q) not in self.pending:
            return []
        link, k = self.pending[self.key(ox, oy, q)]
        group = self.groups[self.group_of[k]]
        self.pending = {key: (l, p) for key, (l, p) in self.pending.items() if l != link or p not in group}
        arrived = self.every.at[pl.ds(0, len(group) * self.unit)]
        return [self.copy(link, k, arrived, arrived)]

    def wait(self, ox, oy, q):
        for c in self.arriving(ox, oy, q):
            c.wait_recv()

    def send(self, stage, only=slice(None)):
        for before, copy in self.forwards(stage, only):
            for c in before:
                c.wait_recv()
            copy.start()

    def forwards(self, stage, only=slice(None)):
        copies = []
        todo = [(link, pieces_of(link)) for link in range(4)]
        count = len(todo[0][1][stage])
        for i in range(count)[only]:
            for link, stages in todo:
                k = sum(len(s) for s in stages[:stage]) + i
                ox, oy, q = stages[stage][i]
                place = self.place(ox, oy, q)
                if (ox, oy) == (0, 0):
                    before, source = [], self.own.at[pl.ds(q * self.unit, self.unit)]
                else:
                    before, source = self.arriving(ox, oy, q), place
                copies.append((before, self.copy(link, k, source, place)))
                self.sent[link] += 1
        return copies

    def wait_shard(self, ox, oy):
        for q in range(4):
            self.wait(ox, oy, q)

    def finish_sends(self):
        for link, count in enumerate(self.sent):
            if count:
                sent = self.every.at[pl.ds(0, count * self.unit)]
                self.copy(link, 0, sent, sent).wait_send()
        self.sent = [0] * 4

    def finish(self):
        for key in list(self.pending):
            self.wait(*key)
        self.finish_sends()


UP_DOWN = {"y": (2, 3), "x": (0, 1)}


def blocks_of(axis):
    up, down = UP_DOWN[axis]
    high, low = (0, 1) if axis == "y" else (2, 3)
    return {
        high: [(2, "relay", up), (1, "later", up), (-1, "direct", down), (0, "own", high)],
        low: [(2, "relay", down), (-1, "later", down), (1, "direct", up), (0, "own", low)],
    }


def barrier_with_neighbours(torus):
    barrier = pltpu.get_barrier_semaphore()
    for offset in STEPS:
        pl.semaphore_signal(barrier, inc=1, device_id={"tp": torus.at(*offset)}, device_id_type=MESH)
    pl.semaphore_wait(barrier, len(STEPS))


def run(copies):
    for c in copies:
        c.start()
    for c in copies:
        c.wait()


def gather_kernel(side, x_ref, dy_ref, pre_ref, w_down_ref, w_in_ref, x_all, dy_all, hidden_ref, d_pre_ref, dw_down_ref, *rest):
    relay, direct, direct_last, later, own_terms = (rest[4 * i : 4 * i + 4] for i in range(5))
    (
        weights, stage, dy_buf, pre_buf, hidden_buf, d_pre, narrow, wide, dy_tile,
        x_send, x_recv, dy_send, dy_recv, load_sem, store_sem, stage_sem, block_sem, tile_sem, out_sem,
    ) = rest[20:]
    rows, depth = dy_ref.shape
    width = pre_ref.shape[1]
    quarter = depth // 4
    torus = Torus(side)
    barrier_with_neighbours(torus)

    dys = Gather(dy_ref, dy_all, dy_send, dy_recv, torus, APART)
    xs = Gather(x_ref, x_all, x_send, x_recv, torus, TOGETHER)
    dys.send(0)

    def load_quarter(q):
        return pltpu.make_async_copy(w_in_ref.at[pl.ds(q * quarter, quarter)], stage, stage_sem)

    def tile_at(n, size=TILE):
        return pl.ds(n * size if isinstance(n, int) else pl.multiple_of(n * size, size), size)

    load_quarter(0).start()

    @pl.loop(0, width // TILE)
    def _(n):
        run([pltpu.make_async_copy(w_down_ref.at[tile_at(n)], dy_buf.at[pl.ds(0, TILE)], load_sem.at[0])])
        for k in range(4):
            weights[k, :, tile_at(n)] = dy_buf[0:TILE, k * quarter : (k + 1) * quarter].T

    def rows_of(ox, oy):
        return pl.ds(pl.multiple_of(torus.at(ox, oy) * rows, rows), rows)

    def wrap(offset):
        return offset % side if isinstance(offset, int) else lax.rem(offset + side, side)

    half = [pl.ds(0, rows), pl.ds(rows, rows)]
    stores = []

    def step_hidden(*pair, own=None):
        here = [rows_of(*offset) for offset in pair]
        at = [d_pre.at[wrap(ox), wrap(oy)] for ox, oy in pair]
        count = range(len(pair))
        run(
            [
                pltpu.make_async_copy(dy_ref if i == own else dy_all.at[here[i]], dy_buf.at[half[i]], load_sem.at[i])
                for i in count
            ]
            + [pltpu.make_async_copy(pre_ref.at[here[i]], pre_buf.at[half[i]], load_sem.at[2 + i]) for i in count]
        )
        flush()
        used = slice(0, len(pair) * rows)

        @pl.loop(0, width // TILE)
        def _(n):
            tile = tile_at(n)
            d_hidden = jnp.dot(
                dy_buf[used, :], weights[:, :, tile].reshape(depth, TILE), preferred_element_type=jnp.float32
            )
            hidden, back = jax.vjp(act, pre_buf[used, tile].astype(jnp.float32))
            hidden_buf[used, tile] = hidden.astype(hidden_buf.dtype)
            grad = back(d_hidden)[0].astype(d_pre.dtype)
            for i in count:
                at[i][:, tile] = grad[i * rows : (i + 1) * rows]

        for i in count:
            stores.append(pltpu.make_async_copy(hidden_buf.at[half[i]], hidden_ref.at[here[i]], store_sem.at[i]))
            stores.append(pltpu.make_async_copy(at[i], d_pre_ref.at[here[i]], store_sem.at[2 + i]))
            if i == own:
                stores.append(pltpu.make_async_copy(dy_buf.at[half[i]], dy_all.at[here[i]], store_sem.at[4]))
        for c in stores:
            c.start()

    def flush():
        for c in stores:
            c.wait()
        stores.clear()

    def steps_hidden(pair):
        flush()

        @pl.loop(0, 2)
        def _(k):
            step_hidden(*pair(k))
            flush()

    leaving = {0: [], 1: []}

    def step_dx(axis, q, offset, kind, index):
        exact = kind in ("later", "own")
        buf, which = (wide, 0) if exact else (narrow, 1)
        for c in leaving[which]:
            c.wait()

        @pl.loop(0, quarter // TILE)
        def _(n):
            tile = tile_at(n)
            lines = d_pre[:, offset % side] if axis == "y" else d_pre[offset % side]
            term = jnp.dot(lines.reshape(side * rows, width), weights[q, :, tile], preferred_element_type=jnp.float32)
            buf[:, :, tile] = term.astype(buf.dtype).reshape(side, rows, TILE)

        if kind == "direct":
            cut = [(buf.at[pl.ds(1, side - 1)], direct[index]), (buf.at[0], direct_last[index])]
        else:
            cut = [(buf, {"relay": relay, "later": later, "own": own_terms}[kind][index])]
        leaving[which] = [pltpu.make_async_copy(*c, block_sem.at[which, i]) for i, c in enumerate(cut)]
        for c in leaving[which]:
            c.start()

    dys.send(1)
    dys.send(2)
    step_hidden((0, 0), own=0)
    for offset in STEPS:
        dys.wait_shard(*offset)
    steps_hidden(lambda k: ((1 - k, k), (k - 1, -k)))
    dys.send(3)
    dys.send(4, slice(0, 3))
    for s in (1, -1):
        for offset in ((1, s), (-1, s)):
            dys.wait_shard(*offset)
        step_hidden((1, s), (-1, s))
        if s == 1:
            dys.send(4, slice(3, 4))
            xs.send(0)
    for shards in (((2, 0), (0, 2)), ((2, -1), (-1, 2)), ((2, 1), (1, 2)), ((2, 2),)):
        for offset in shards:
            dys.wait_shard(*offset)
        step_hidden(*shards)
    flush()
    own = dy_buf.at[half[0]]
    run([pltpu.make_async_copy(x_ref, own, load_sem.at[0])])
    stores.append(pltpu.make_async_copy(own, x_all.at[rows_of(0, 0)], store_sem.at[0]))
    stores[-1].start()
    tiles = dy_tile.shape[-1]

    def load_tile(n, slot):
        return pltpu.make_async_copy(dy_all.at[:, tile_at(n, tiles)], dy_tile.at[slot], tile_sem.at[slot])

    def store_tile(n, slot):
        return pltpu.make_async_copy(stage.at[:, tile_at(slot, tiles)], dw_down_ref.at[:, tile_at(n, tiles)], out_sem.at[slot])

    spare = side * side * rows - quarter
    hidden_loads = [
        pltpu.make_async_copy(hidden_ref.at[pl.ds(0, quarter)], weights.at[0], load_sem.at[1]),
        pltpu.make_async_copy(hidden_ref.at[pl.ds(quarter, spare)], weights.at[1, pl.ds(0, spare)], load_sem.at[2]),
    ]
    for axis in ("y", "x"):
        for q, blocks in blocks_of(axis).items():
            load_quarter(q).wait()

            @pl.loop(0, quarter // TILE)
            def _(n):
                weights[q, :, tile_at(n)] = stage[tile_at(n), :].T

            if q < 3:
                load_quarter(q + 1).start()
            else:
                for c in hidden_loads + [load_tile(0, 0)]:
                    c.start()
            for offset, kind, index in blocks:
                step_dx(axis, q, offset, kind, index)
            if q == 0:
                xs.send(1)
                xs.send(2)
            if q == 2:
                xs.send(3)
    for c in hidden_loads:
        c.wait()
    count = depth // tiles
    forwards = {4: xs.forwards(4, slice(0, 3)), 7: xs.forwards(4, slice(3, 4))}

    @pl.loop(0, count)
    def _(n):
        slot = lax.rem(n, 2)

        for when, copies in forwards.items():

            @pl.when(n == when)
            def _():
                for before, copy in copies:
                    for c in before:
                        c.wait_recv()
                    copy.start()

        @pl.when(n + 1 < count)
        def _():
            load_tile(n + 1, 1 - slot).start()

        @pl.when(n >= 2)
        def _():
            store_tile(n - 2, slot).wait()

        load_tile(n, slot).wait()
        hidden = jnp.concatenate([weights[0], weights[1, 0:spare, :]], axis=0)
        stage[:, tile_at(slot, tiles)] = lax.dot_general(
            hidden, dy_tile[slot], (((0,), (0,)), ((), ())), preferred_element_type=jnp.float32
        ).astype(stage.dtype)
        store_tile(n, slot).start()

    for c in stores + leaving[0] + leaving[1]:
        c.wait()
    for n in (count - 2, count - 1):
        store_tile(n, n % 2).wait()
    dys.finish()
    xs.finish_sends()
    xs.finish()


def gather_and_differentiate(x, dy, pre, w_down, w_in, group):
    side = math.isqrt(group)
    assert side == 4 and side * side == group
    rows, depth = dy.shape
    width = pre.shape[1]
    quarter, tile = depth // 4, 2 * TILE
    assert rows % 32 == 0 and width % TILE == 0 and quarter % TILE == 0 and depth // tile > 7
    assert quarter < group * rows <= 2 * quarter and width == quarter
    like = jax.ShapeDtypeStruct
    any_space = pl.BlockSpec(memory_space=pl.ANY)
    block = (side, rows, quarter)
    dma = pltpu.SemaphoreType.DMA
    outs = pl.pallas_call(
        functools.partial(gather_kernel, side),
        out_shape=[like((group * rows, depth), x.dtype)] * 2
        + [like((group * rows, width), x.dtype)] * 2
        + [like((width, depth), x.dtype)]
        + [like(block, x.dtype)] * 4
        + [like((side - 1, *block[1:]), x.dtype)] * 4
        + [like(block[1:], x.dtype)] * 4
        + [like(block, jnp.float32)] * 8,
        in_specs=[any_space] * 5,
        out_specs=[any_space] * 25,
        scratch_shapes=[
            pltpu.VMEM((4, quarter, width), x.dtype),
            pltpu.VMEM((quarter, width), x.dtype),
            pltpu.VMEM((2 * rows, depth), x.dtype),
            pltpu.VMEM((2 * rows, width), x.dtype),
            pltpu.VMEM((2 * rows, width), x.dtype),
            pltpu.VMEM((side, side, rows, width), x.dtype),
            pltpu.VMEM(block, x.dtype),
            pltpu.VMEM(block, jnp.float32),
            pltpu.VMEM((2, group * rows, tile), x.dtype),
            dma((4,)),
            dma((4, len(TOGETHER))),
            dma((4,)),
            dma((4, len(APART))),
            dma((4,)),
            dma((5,)),
            dma,
            dma((2, 2)),
            dma((2,)),
            dma((2,)),
        ],
        compiler_params=pltpu.CompilerParams(
            collective_id=0, has_side_effects=True, vmem_limit_bytes=67_043_328
        ),
        cost_estimate=pl.CostEstimate(
            flops=6 * group * rows * depth * width,
            bytes_accessed=2 * (group * rows * (7 * depth + 4 * width) + 3 * depth * width),
            transcendentals=0,
        ),
        name="gather_and_differentiate",
    )(x, dy, pre, w_down, w_in)
    return *outs[:5], *(outs[5 + 4 * i : 9 + 4 * i] for i in range(5))


def shift(value, link, mesh):
    group = mesh.shape["tp"]
    side = math.isqrt(group)
    dx, dy = STEPS[link]
    pairs = []
    for g in range(mesh.shape["dp"]):
        index = (lambda x, y: -y % side * side + -x % side) if g % 2 else (lambda x, y: x * side + y)
        pairs += [
            (g * group + index(x, y), g * group + index((x + dx) % side, (y + dy) % side))
            for x in range(side)
            for y in range(side)
        ]
    return lax.ppermute(value, ("dp", "tp"), pairs)


def links_of_quarters():
    takes = {}
    for axis, other in (("y", "x"), ("x", "y")):
        (up, down), (cross_up, cross_down) = UP_DOWN[axis], UP_DOWN[other]
        high, low = (0, 1) if axis == "y" else (2, 3)
        takes[high] = up, down, cross_up, cross_down
        takes[low] = down, up, cross_down, cross_up
    return takes


def scatter_kernel(side, *refs):
    relay, direct, later, own_terms = (refs[4 * i : 4 * i + 4] for i in range(4))
    (
        kept_ref, last_ref, later_got, cross_got, later_out, cross_out, exact_in, narrow_in, sums,
        later_send, later_recv, cross_send, cross_recv, exact_sem, narrow_sem,
    ) = refs[16:]
    rows, quarter = exact_in.shape[1:]
    torus = Torus(side)
    barrier_with_neighbours(torus)

    def remote(link, source, target, send_sem, recv_sem):
        return pltpu.make_async_remote_copy(
            src_ref=source,
            dst_ref=target,
            send_sem=send_sem,
            recv_sem=recv_sem,
            device_id={"tp": torus.at(*STEPS[link])},
            device_id_type=MESH,
        )

    later_copies = {
        (link, j): remote(link, later_out.at[link, j], later_got.at[link, j], later_send.at[link], later_recv.at[link, j])
        for link in range(4)
        for j in range(side)
    }
    takes = links_of_quarters()
    step = lambda link: 1 if link in (0, 2) else side - 1
    columns = [pl.ds(q * quarter, quarter) for q in range(4)]
    cross_copies = {
        (q, k): remote(
            takes[q][3 if k == 1 else 2],
            cross_out.at[q, k],
            last_ref.at[:, columns[q]] if k == 2 else cross_got.at[q, k],
            cross_send.at[q],
            cross_recv.at[q, k],
        )
        for q in range(4)
        for k in range(3)
    }

    def add(target, *parts):
        strip = 16

        @pl.loop(0, rows // strip)
        def _(i):
            at = pl.ds(pl.multiple_of(i * strip, strip), strip)
            total = parts[0][at, :].astype(jnp.float32)
            for part in parts[1:]:
                total = total + part[at, :].astype(jnp.float32)
            target[at, :] = total.astype(target.dtype)

    order = [2, 1, side - 1, 0]
    tasks = [("later", link, j, later[link].at[j], relay[link].at[j]) for j in order for link in range(4)]
    for j in order:
        for q in range(4):
            link = takes[q][1]
            tasks.append(("sum", q, j, own_terms[q].at[j], None if j == 0 else direct[link].at[j - 1]))
    slots = exact_in.shape[0]

    def loads(n):
        _, _, _, exact, narrow = tasks[n]
        slot = n % slots
        copies = [pltpu.make_async_copy(exact, exact_in.at[slot], exact_sem.at[slot])]
        if narrow is not None:
            copies.append(pltpu.make_async_copy(narrow, narrow_in.at[slot], narrow_sem.at[slot]))
        return copies

    for n in range(slots - 1):
        for c in loads(n):
            c.start()
    for n, (kind, which, j, _, narrow) in enumerate(tasks):
        if n + slots - 1 < len(tasks):
            for c in loads(n + slots - 1):
                c.start()
        for c in loads(n):
            c.wait()
        exact, slot = exact_in.at[n % slots], n % slots
        if kind == "later":
            add(later_out.at[which, j], exact, narrow_in.at[slot])
            later_copies[which, j].start()
            continue
        q = which
        main, _, _, near_link = takes[q]
        later_copies[main, j].wait_recv()
        parts = [exact, later_got.at[main, j]]
        if narrow is not None:
            parts.append(narrow_in.at[slot])
        if j == 2:
            add(cross_out.at[q, 0], *parts)
            cross_copies[q, 0].start()
        elif j == step(near_link):
            add(cross_out.at[q, 1], *parts)
            cross_copies[q, 1].start()
        else:
            add(sums.at[q, 0 if j == 0 else 1], *parts)
    for q in range(4):
        cross_copies[q, 0].wait_recv()
        add(cross_out.at[q, 2], sums.at[q, 1], cross_got.at[q, 0])
        cross_copies[q, 2].start()
    for q in range(4):
        cross_copies[q, 1].wait_recv()
        add(kept_ref.at[:, columns[q]], sums.at[q, 0], cross_got.at[q, 1])
    for link in range(4):
        remote(link, later_out.at[link], later_out.at[link], later_send.at[link], later_recv.at[link, 0]).wait_send()
    for q in range(4):
        remote(takes[q][2], cross_out.at[q], cross_out.at[q], cross_send.at[q], cross_recv.at[q, 0]).wait_send()
    for q in range(4):
        cross_copies[q, 2].wait_recv()


def sum_and_scatter(relay, direct, later, own_terms):
    side, rows, quarter = relay[0].shape
    kind = relay[0].dtype
    any_space = pl.BlockSpec(memory_space=pl.ANY)
    dma = pltpu.SemaphoreType.DMA
    piece, slots = (rows, quarter), 4
    return pl.pallas_call(
        functools.partial(scatter_kernel, side),
        out_shape=[pltpu.VMEM((rows, 4 * quarter), t) for t in (jnp.float32, kind)],
        in_specs=[any_space] * 16,
        out_specs=[pl.BlockSpec(memory_space=pltpu.VMEM)] * 2,
        scratch_shapes=[
            pltpu.VMEM((4, side, *piece), kind),
            pltpu.VMEM((4, 2, *piece), kind),
            pltpu.VMEM((4, side, *piece), kind),
            pltpu.VMEM((4, 3, *piece), kind),
            pltpu.VMEM((slots, *piece), jnp.float32),
            pltpu.VMEM((slots, *piece), kind),
            pltpu.VMEM((4, 2, *piece), jnp.float32),
            dma((4,)),
            dma((4, side)),
            dma((4,)),
            dma((4, 3)),
            dma((slots,)),
            dma((slots,)),
        ],
        compiler_params=pltpu.CompilerParams(
            collective_id=1, has_side_effects=True, vmem_limit_bytes=54 * 1024 * 1024
        ),
        cost_estimate=pl.CostEstimate(
            flops=8 * side * rows * quarter, bytes_accessed=60 * side * rows * quarter, transcendentals=0
        ),
        name="sum_and_scatter",
    )(*relay, *direct, *later, *own_terms)


def finish_kernel(kept_ref, last_ref, *refs):
    direct, (dx_ref, owner, dx, owner_sem, dx_sem) = refs[:4], refs[4:]
    quarter = owner.shape[2]
    columns = [pl.ds(q * quarter, quarter) for q in range(4)]
    loads = [
        [
            pltpu.make_async_copy(direct[q], owner.at[q], owner_sem.at[q]),
        ]
        for q in range(4)
    ]
    for copies in loads:
        for c in copies:
            c.start()
    stores = []
    for q, copies in enumerate(loads):
        for c in copies:
            c.wait()
        total = kept_ref[:, columns[q]] + owner[q].astype(jnp.float32) + last_ref[:, columns[q]].astype(jnp.float32)
        dx[q] = total.astype(dx.dtype)
        stores.append(pltpu.make_async_copy(dx.at[q], dx_ref.at[:, columns[q]], dx_sem.at[q]))
        stores[-1].start()
    for c in stores:
        c.wait()


def finish_dx(kept, last, direct_last):
    rows, depth = kept.shape
    pieces = (4, rows, depth // 4)
    takes = links_of_quarters()
    any_space = pl.BlockSpec(memory_space=pl.ANY)
    return pl.pallas_call(
        finish_kernel,
        in_specs=[pl.BlockSpec(memory_space=pltpu.VMEM)] * 2 + [any_space] * 4,
        out_specs=any_space,
        out_shape=jax.ShapeDtypeStruct(kept.shape, last.dtype),
        scratch_shapes=[pltpu.VMEM(pieces, last.dtype)] * 2 + [pltpu.SemaphoreType.DMA((4,))] * 2,
        compiler_params=pltpu.CompilerParams(vmem_limit_bytes=32 * 1024 * 1024),
        cost_estimate=pl.CostEstimate(flops=2 * rows * depth, bytes_accessed=10 * rows * depth, transcendentals=0),
        name="finish_dx",
    )(kept, last, *(direct_last[takes[q][1]] for q in range(4)))


def solution(mesh):
    group = mesh.shape["tp"]

    def step(x, dy, pre, w_in, w_down):
        x_all, _, _, d_pre, dw_down, relay, direct, direct_last, later, own_terms = gather_and_differentiate(
            x, dy, pre, w_down, w_in, group
        )
        relay = [shift(block, link, mesh) for link, block in enumerate(relay)]
        direct = [shift(block, link, mesh) for link, block in enumerate(direct)]
        direct_last = [shift(block, link, mesh) for link, block in enumerate(direct_last)]
        dw_in, dw_down = dw_in_and_copy(x_all, d_pre, dw_down, 2 * TILE)
        dw_in, dw_down, later = lax.optimization_barrier((dw_in, dw_down, later))
        dx = finish_dx(*sum_and_scatter(relay, direct, later, own_terms), direct_last)
        return dx, dw_in, dw_down

    tokens = P(("dp", "tp"), None)
    step = jax.shard_map(
        step,
        mesh=mesh,
        in_specs=(tokens, tokens, P("dp", "tp"), P(None, "tp"), P("tp", None)),
        out_specs=(tokens, P("dp", "tp"), tokens),
        check_vma=False,
    )
    return step
```
